32 devices in a mesh: gx: 8 (over y, x, core), gy: 4 (over z).
Axes of the slice: x: 2, y: 2, z: 4, core: 2. Of those that a mesh axis runs over, the one named last changes fastest.
Arguments:
- features: bfloat16 [32, 16, 128, 128], P(None, 'gx', 'gy'), may hold values from -80 to 80
- kernel_one: bfloat16 [32, 32, 3, 3, 3], replicated, may hold values from -0.21875 to 0.21875
- gain_one: float32 [32], replicated, may hold values from 0.5 to 1.5
- bias_one: float32 [32], replicated, may hold values from -0.5 to 0.5
- kernel_two: bfloat16 [32, 32, 3, 3, 3], replicated, may hold values from -0.21875 to 0.21875
- gain_two: float32 [32], replicated, may hold values from 0.5 to 1.5
- bias_two: float32 [32], replicated, may hold values from -0.5 to 0.5
- cotangent: bfloat16 [32, 16, 128, 128], P(None, 'gx', 'gy'), may hold values from -80 to 80
Outputs:
- output: bfloat16 [32, 16, 128, 128], P(None, 'gx', 'gy')
- features_grad: bfloat16 [32, 16, 128, 128], P(None, 'gx', 'gy')
- kernel_one_grad: float32 [32, 32, 3, 3, 3], replicated
- kernel_two_grad: float32 [32, 32, 3, 3, 3], replicated
- norm_grads: float32 [4, 32], replicated
The draws below stay inside these ranges and needn't reach their ends.
All inputs are finite; a program needn't handle non-finite values.
Results may differ from the reference program's by a relative error of at most 0.0078.
Values may be sent and summed in bfloat16 or wider, within the bound.
A program may use at most 192 MiB of HBM per device.

```python
import jax
import jax.numpy as jnp
from jax import lax

C = 32
NX = 16
NY = 128
NZ = 128


def scaled_volume(key, salt):
    key = jax.random.fold_in(key, salt)
    noise_key, offset_key, rough_key = jax.random.split(key, 3)
    offsets = jax.random.uniform(offset_key, (C, 1, 1, 1), jnp.float32, -1.0, 1.0)
    rough = jnp.exp(jax.random.uniform(rough_key, (C, NX, NY, NZ), jnp.float32, jnp.log(0.5), jnp.log(2.0)))
    place_x = jnp.arange(NX, dtype=jnp.float32) / NX
    place_y = jnp.arange(NY, dtype=jnp.float32) / NY
    noise = jnp.clip(jax.random.normal(noise_key, (C, NX, NY, NZ), jnp.float32), -4.0, 4.0)
    ramp = jnp.exp(jnp.log(3.0) * place_x)[:, None] * jnp.exp(jnp.log(2.0) * place_y)[None, :]
    return (noise + offsets) * rough * ramp[None, :, :, None]


def draw_features(key, part):
    return scaled_volume(key, 11).astype(jnp.bfloat16)


def draw_cotangent(key, part):
    return scaled_volume(key, 23).astype(jnp.bfloat16)


def scatter_about(stream_key, extent, width, limit, kind=jnp.bfloat16):
    drawn = width * jax.random.normal(stream_key, extent, jnp.float32)
    return jnp.clip(drawn, min=-limit, max=limit).astype(kind)


def setup_inputs(seed: int = 0) -> dict:
    keys = jax.random.split(jax.random.key(seed), 9)
    return {
        "features": draw_features(jax.random.fold_in(keys[8], 71), 0),
        "kernel_one": scatter_about(keys[1], (C, C, 3, 3, 3), (C * 27) ** -0.5, 0.21875),
        "gain_one": jnp.clip(1.0 + 0.1 * jax.random.normal(keys[2], (C,), jnp.float32), 0.5, 1.5),
        "bias_one": jnp.clip(jax.random.uniform(keys[3], (C,), jnp.float32, -0.5, 0.5), -0.5, 0.5),
        "kernel_two": scatter_about(keys[4], (C, C, 3, 3, 3), (C * 27) ** -0.5, 0.21875),
        "gain_two": jnp.clip(1.0 + 0.1 * jax.random.normal(keys[5], (C,), jnp.float32), 0.5, 1.5),
        "bias_two": jnp.clip(jax.random.uniform(keys[6], (C,), jnp.float32, -0.5, 0.5), -0.5, 0.5),
        "cotangent": draw_cotangent(jax.random.fold_in(keys[8], 71), 0),
    }


EPSILON = 1e-05
SLOPE = 0.01
SHARPNESS = 8.0

def activate(shifted):
    return SLOPE * shifted + (1.0 - SLOPE) * jax.nn.softplus(SHARPNESS * shifted) / SHARPNESS

def activate_slope(shifted):
    return SLOPE + (1.0 - SLOPE) * jax.nn.sigmoid(SHARPNESS * shifted)

def column(values):
    return values[:, None, None, None]

def pad_all(values):
    return jnp.pad(values, ((0, 0), (1, 1), (1, 1), (1, 1)))

def conv_valid(padded, kernel):
    result = lax.conv_general_dilated(padded[None], kernel, (1, 1, 1), 'VALID', dimension_numbers=('NCDHW', 'OIDHW', 'NCDHW'), preferred_element_type=jnp.float32)
    return result[0]

def flip_kernel(kernel):
    return jnp.transpose(kernel[:, :, ::-1, ::-1, ::-1], (1, 0, 2, 3, 4))

def weight_grad(padded, gradient):
    result = lax.conv_general_dilated(padded[:, None], gradient[:, None], (1, 1, 1), 'VALID', dimension_numbers=('NCDHW', 'OIDHW', 'NCDHW'), preferred_element_type=jnp.float32)
    return jnp.transpose(result, (1, 0, 2, 3, 4))

def normalize(hidden, total_cells):
    center = lax.optimization_barrier(jnp.sum(hidden, axis=(1, 2, 3))) / total_cells
    spread = lax.optimization_barrier(jnp.sum(jnp.square(hidden - column(center)), axis=(1, 2, 3))) / total_cells
    inverse_std = lax.rsqrt(spread + EPSILON)
    return ((hidden - column(center)) * column(inverse_std), inverse_std)

def norm_backward(slope, normed, gain, inverse_std, total_cells):
    sum_plain = lax.optimization_barrier(jnp.sum(slope, axis=(1, 2, 3)))
    sum_normed = lax.optimization_barrier(jnp.sum(slope * normed, axis=(1, 2, 3)))
    gradient = column(gain * inverse_std) * (slope - column(sum_plain / total_cells) - normed * column(sum_normed / total_cells))
    return (gradient.astype(jnp.bfloat16), sum_plain, sum_normed)

def reference(features, kernel_one, gain_one, bias_one, kernel_two, gain_two, bias_two, cotangent):
    total_cells = float(NX * NY * NZ)
    x_pad = pad_all(features)
    normed_one, inv_one = normalize(conv_valid(x_pad, kernel_one), total_cells)
    shifted_one = normed_one * column(gain_one) + column(bias_one)
    active = activate(shifted_one).astype(jnp.bfloat16)
    a_pad = pad_all(active)
    normed_two, inv_two = normalize(conv_valid(a_pad, kernel_two), total_cells)
    shifted_two = normed_two * column(gain_two) + column(bias_two)
    output = activate(shifted_two).astype(jnp.bfloat16)
    slope_two = cotangent.astype(jnp.float32) * activate_slope(shifted_two)
    grad_two, plain_two, nsum_two = norm_backward(slope_two, normed_two, gain_two, inv_two, total_cells)
    scale = 1.0 / jnp.sqrt(jnp.float32(total_cells))
    kernel_two_grad = weight_grad(a_pad, grad_two) * scale
    back_one = conv_valid(pad_all(grad_two), flip_kernel(kernel_two))
    slope_one = back_one * activate_slope(shifted_one)
    grad_one, plain_one, nsum_one = norm_backward(slope_one, normed_one, gain_one, inv_one, total_cells)
    kernel_one_grad = weight_grad(x_pad, grad_one) * scale
    features_grad = conv_valid(pad_all(grad_one), flip_kernel(kernel_one)).astype(jnp.bfloat16)
    norm_grads = jnp.stack([nsum_one, plain_one, nsum_two, plain_two]) * scale
    return (output, features_grad, kernel_one_grad, kernel_two_grad, norm_grads)
```

```python
import functools

import jax
import jax.numpy as jnp
from jax import lax
from jax.experimental import pallas as pl
from jax.experimental.pallas import tpu as pltpu
from jax.sharding import PartitionSpec as P

EPSILON = 1e-05
SLOPE = 0.01
SHARPNESS = 8.0
MESH = pl.DeviceIdType.MESH
F32 = jnp.float32
BF16 = jnp.bfloat16
L = 128
CH = 4
FEAT, COT, HID1, HID2, SLO1 = range(5)
NEXCH = 5
NT = (((1,), (1,)), ((), ()))


def activate(s):
    scaled = SHARPNESS * s
    soft = jnp.maximum(scaled, 0.0) + jnp.log(1.0 + jnp.exp(-jnp.abs(scaled)))
    return SLOPE * s + ((1.0 - SLOPE) / SHARPNESS) * soft


def activate_slope(s):
    half = 0.5 * (1.0 - SLOPE)
    return (SLOPE + half) + half * jnp.tanh((0.5 * SHARPNESS) * s)


def kernel(
    nx, ny, total,
    f_ref, c_ref, k1_ref, k2_ref, g1_ref, b1_ref, g2_ref, b2_ref,
    o_ref, fg_ref, dk1_ref, dk2_ref, ng_ref,
    t1, par, e_mat, s_mat, i_mat, base, wf1, wf2, wb2, wb1,
    vo_f, vh_f, vo_c, vh_c, vo_a, vh_a, vo_g, vh_g, vt_f, vt_a,
    hc1, hc2, n1o, n1h, n2o, n2h, s2o, s2h, s1o, outb, bs, mcs, scs, mcs1, raw,
    spr, spl, se, rl, rr, re, rdl, rdr, hs_sem, hr_sem,
    msg, st, ss_sem, sr_sem,
    pk, rsb, ags, agb, ws_sem, wr_sem,
):
    C, X, Y, Z = f_ref.shape
    R = Z // 2
    CR = CH * R
    NCH = Y // CH
    n = nx * ny
    PIECE = rsb.shape[2]
    gx, gy = lax.axis_index("gx"), lax.axis_index("gy")
    me = gx * ny + gy
    has_l, has_r = gx > 0, gx < nx - 1
    has_d, has_u = gy > 0, gy < ny - 1

    def coords(d):
        return (d // ny, lax.rem(d, ny))

    barrier = pltpu.get_barrier_semaphore()

    def hello(k, carry):
        pl.semaphore_signal(
            barrier, inc=1, device_id=coords(lax.rem(me + k, n)), device_id_type=MESH
        )
        return carry

    lax.fori_loop(1, n, hello, 0)

    lane = lax.broadcasted_iota(jnp.int32, (1, L), 1)
    xb = lax.rem(lane // C, 2) == 1
    z0 = lane < L // 2
    flag = lambda b: jnp.where(b, 1, 0)
    keep_h = jnp.where(xb, flag(has_l), flag(has_r)) > 0
    full_y = jnp.full((1, L), 1, jnp.int32)
    keep_o = [full_y * flag(has_d) > 0, full_y * flag(has_u) > 0]
    keep_ho = [(jnp.where(xb, flag(has_l), flag(has_r)) * flag(b)) > 0 for b in (has_d, has_u)]

    def row_of(y):
        return pl.multiple_of(y * R, R)

    def fold(v):
        v = v + pltpu.roll(v, C, 1)
        return v + pltpu.roll(v, 2 * C, 1)

    def eight(v):
        return jnp.sum(v.reshape(v.shape[0] // 8, 8, L), axis=0)

    def one(v):
        return jnp.sum(v, axis=0, keepdims=True)

    r_i = lax.broadcasted_iota(jnp.int32, (R, 2 * Z), 0)
    c_i = lax.broadcasted_iota(jnp.int32, (R, 2 * Z), 1)
    e_mat[...] = jnp.where(
        lax.rem(c_i, Z) == 2 * r_i + c_i // Z, 1.0, 0.0
    ).astype(BF16)
    r_i = lax.broadcasted_iota(jnp.int32, (2 * L, 2 * Z), 0)
    c_i = lax.broadcasted_iota(jnp.int32, (2 * L, 2 * Z), 1)
    same = lax.rem(r_i // R, 2) == c_i // Z
    s_mat[...] = jnp.where(
        same & (lax.rem(c_i, Z) == 2 * lax.rem(r_i, R) + r_i // L), 1.0, 0.0
    ).astype(BF16)
    r_i = lax.broadcasted_iota(jnp.int32, (L, L), 0)
    c_i = lax.broadcasted_iota(jnp.int32, (L, L), 1)
    i_mat[...] = jnp.where(r_i == c_i, 1.0, 0.0).astype(BF16)
    par[...] = jnp.zeros(par.shape, F32)
    for row, ref in enumerate((g1_ref, b1_ref, g2_ref, b2_ref)):
        par[row : row + 1, 0:C] = ref[...]
    params = fold(par[...])
    gain1, bias1, gain2, bias2 = [params[r : r + 1] for r in range(4)]
    bs[...] = jnp.zeros(bs.shape, F32)

    spots_in = [(0, 0, z, x) for z in range(2) for x in range(2)]
    halo_x = {0: 2, 1: -1}
    rows_in = [(x, z) for _, _, z, x in spots_in] + [(halo_x[x], z) for _, _, z, x in spots_in]
    cols_a = [(x, z) for _, _, z, x in spots_in]
    cols_b = [(x, 2 if z == 0 else -1) for _, _, z, x in spots_in]

    def build(k_ref, w_ref, forward):
        if forward:
            stacked = jnp.concatenate([k_ref[t] for t in range(27) for _ in range(4)], axis=0)
            wide = lax.dot_general(
                i_mat[0:C, 0:C], stacked, NT, preferred_element_type=F32
            )
            for t in range(27):
                base[t] = wide[:, t * L : (t + 1) * L]
        else:
            r4 = lax.broadcasted_iota(jnp.int32, (C, L), 0)
            c4 = lax.rem(lax.broadcasted_iota(jnp.int32, (C, L), 1), C)
            spread4 = jnp.where(r4 == c4, 1.0, 0.0).astype(BF16)
            tall = k_ref[...].reshape(27 * C, C)
            wide = jnp.dot(tall, spread4, preferred_element_type=F32)
            for t in range(27):
                base[t] = wide[t * C : (t + 1) * C]
        block = lax.broadcasted_iota(jnp.int32, (C, L), 1) // C

        def one_row(j, carry):
            dy = j if forward else 2 - j
            for kb, (xi, zi) in enumerate(rows_in):
                for t, cols in enumerate((cols_a, cols_b)):
                    value = jnp.zeros((C, L), F32)
                    for b, (xo, zo) in enumerate(cols):
                        dx, dz = xi - xo + 1, zi - zo + 1
                        if not forward:
                            dx, dz = 2 - dx, 2 - dz
                        if 0 <= dx <= 2 and 0 <= dz <= 2:
                            tap = base[dx * 9 + dy * 3 + dz]
                            value = jnp.where(block == b, tap, value)
                    w_ref[j, kb * C : (kb + 1) * C, t * L : (t + 1) * L] = value.astype(BF16)
            return carry

        lax.fori_loop(0, 3, one_row, 0)

    def enter(in_ref, vo, e):
        def widen(c, carry):
            t1[pl.ds(pl.multiple_of(c * X * Y, X * Y), X * Y), :] = (
                in_ref[c].reshape(X * Y, Z).astype(F32)
            )
            return carry

        lax.fori_loop(0, C, widen, 0)
        zero = jnp.zeros((X * C, Z), BF16)

        def chunk(c, carry):
            vs = []
            for k in range(CH):
                y = c * CH + k
                x0 = t1[pl.ds(y, C, stride=X * Y), :]
                x1 = t1[pl.ds(Y + y, C, stride=X * Y), :]
                xy = jnp.concatenate([x0, x1], axis=0).astype(BF16)
                rhs = jnp.concatenate(
                    [jnp.concatenate([xy, zero], axis=1), jnp.concatenate([zero, xy], axis=1)],
                    axis=0,
                )
                v = lax.dot_general(e_mat[...], rhs, NT, preferred_element_type=F32)
                vo[pl.ds(row_of(y + 1), R), :] = v.astype(BF16)
                vs.append(v)
            pack(e, c, vs, None)
            return carry

        lax.fori_loop(0, NCH, chunk, 0)

    def leave(src, dst):
        def pair(p, carry):
            o = src[pl.ds(pl.multiple_of(p * L, L), L), :]
            d = lax.dot_general(i_mat[...], o, NT, preferred_element_type=F32).astype(BF16)
            both = jnp.concatenate([d[: L // 2], d[L // 2 :]], axis=1)
            xs = jnp.dot(both, s_mat[...], preferred_element_type=F32)
            r0 = pl.multiple_of(p * 2 * R, 2 * R)
            t1[pl.ds(r0, R), :] = xs[:, :Z]
            t1[pl.ds(r0 + R, R), :] = xs[:, Z:]
            return carry

        lax.fori_loop(0, Y // 2, pair, 0)

        def channel(c, carry):
            for x in range(X):
                dst[c, x] = t1[pl.ds(x * C + c, Y, stride=X * C), :].astype(BF16)
            return carry

        lax.fori_loop(0, C, channel, 0)

    def flip(vo, vt):
        def pair(p, carry):
            rows = vo[pl.ds(row_of(2 * p + 1), 2 * R), :]
            wide = rows.astype(F32)
            for k in range(2):
                bs[k, 8 : 8 + R, :] = wide[k * R : (k + 1) * R]
            shifted = jnp.concatenate(
                [jnp.where(z0, bs[k, 9 : 9 + R, :], bs[k, 7 : 7 + R, :]) for k in range(2)], axis=0
            ).astype(BF16)
            cols = pl.ds(pl.multiple_of(p * 2 * R, 2 * R), 2 * R)
            for k, part in enumerate((rows, shifted)):
                vt[k * L : (k + 1) * L, cols] = lax.dot_general(
                    i_mat[...], part, NT, preferred_element_type=F32
                ).astype(BF16)
            return carry

        lax.fori_loop(0, Y // 2, pair, 0)

    half = CR // 2

    def pack(e, c, vs, center):
        for p in range(CH // 2):
            a, b = vs[2 * p], vs[2 * p + 1]
            rows = slice(p * (R + 16), p * (R + 16) + R)
            spr[e, c, rows, :] = jnp.where(xb, a, pltpu.roll(b, L - C, 1)).astype(BF16)
            spl[e, c, rows, :] = jnp.where(xb, pltpu.roll(b, C, 1), a).astype(BF16)
        if center is not None:
            center = center.astype(BF16)
            spr[e, c, R : R + 16, :] = center
            spl[e, c, R : R + 16, :] = center

        @pl.when(c == 0)
        def _():
            se[e, 0, 0:R, :] = vs[0].astype(BF16)
            if center is not None:
                se[e, 0, R : R + 16, :] = center

        @pl.when(c == NCH - 1)
        def _():
            se[e, 1, 0:R, :] = vs[CH - 1].astype(BF16)
            if center is not None:
                se[e, 1, R : R + 16, :] = center

    def copy_of(e, index, src, dst, dx, dy):
        return lambda: pltpu.make_async_remote_copy(
            src_ref=src, dst_ref=dst,
            send_sem=hs_sem.at[e, index], recv_sem=hr_sem.at[e, index],
            device_id=(lax.rem(gx + dx + nx, nx), lax.rem(gy + dy + ny, ny)),
            device_id_type=MESH,
        )

    def side_copies(e, c):
        return [
            (has_r, has_l, copy_of(e, c, spr.at[e, c], rl.at[e, c], 1, 0)),
            (has_l, has_r, copy_of(e, NCH + c, spl.at[e, c], rr.at[e, c], -1, 0)),
        ]

    def end_copies(e):
        low, high = pl.ds(0, R + 16), pl.ds(R, R + 16)
        both = jnp.logical_and
        m = 2 * NCH
        last = NCH - 1
        return [
            [
                (has_d, has_u, copy_of(e, m, se.at[e, 0], re.at[e, 1], 0, -1)),
                (both(has_r, has_d), both(has_l, has_u),
                 copy_of(e, m + 2, spr.at[e, 0, low], rdl.at[e, 1], 1, -1)),
                (both(has_l, has_d), both(has_r, has_u),
                 copy_of(e, m + 4, spl.at[e, 0, low], rdr.at[e, 1], -1, -1)),
            ],
            [
                (has_u, has_d, copy_of(e, m + 1, se.at[e, 1], re.at[e, 0], 0, 1)),
                (both(has_r, has_u), both(has_l, has_d),
                 copy_of(e, m + 3, spr.at[e, last, high], rdl.at[e, 0], 1, 1)),
                (both(has_l, has_u), both(has_r, has_d),
                 copy_of(e, m + 5, spl.at[e, last, high], rdr.at[e, 0], -1, 1)),
            ],
        ]

    def start(copies):
        for sends, _, copy in copies:
            @pl.when(sends)
            def _(copy=copy):
                copy().start()

    def arrive(copies):
        for _, takes, copy in copies:
            @pl.when(takes)
            def _(copy=copy):
                copy().wait_recv()

    def send(e, c):
        start(side_copies(e, c))

        @pl.when(c == 0)
        def _():
            start(end_copies(e)[0])

        @pl.when(c == NCH - 1)
        def _():
            start(end_copies(e)[1])

    def send_all(e):
        def body(c, carry):
            send(e, c)
            return carry

        lax.fori_loop(0, NCH, body, 0)

    def arrive_ends(e):
        for copies in end_copies(e):
            arrive(copies)

    def arrive_all(e):
        def body(c, carry):
            arrive(side_copies(e, c))
            return carry

        lax.fori_loop(0, NCH, body, 0)
        arrive_ends(e)

    def sent_all(e):
        def done(copies):
            for sends, _, copy in copies:
                @pl.when(sends)
                def _(copy=copy):
                    copy().wait_send()

        def body(c, carry):
            done(side_copies(e, c))
            return carry

        lax.fori_loop(0, NCH, body, 0)
        for copies in end_copies(e):
            done(copies)

    def center_of(tile):
        wide = tile.astype(F32)
        return (wide[0:8] + wide[8:16])[0:1]

    def halo_rows(e, c):
        center = jnp.where(xb, center_of(rl[e, c, R : R + 16, :]), center_of(rr[e, c, R : R + 16, :]))
        found = []
        for p in range(CH // 2):
            rows = slice(p * (R + 16), p * (R + 16) + R)
            a, b = rl[e, c, rows, :].astype(F32), rr[e, c, rows, :].astype(F32)
            found.append(jnp.where(xb, a, b))
            found.append(jnp.where(xb, pltpu.roll(a, C, 1), pltpu.roll(b, L - C, 1)))
        return found, center

    def end_rows(e, side):
        own, own_center = re[e, side, 0:R, :].astype(F32), center_of(re[e, side, R : R + 16, :])
        data, tile = (slice(16, 16 + R), slice(0, 16)) if side == 0 else (slice(0, R), slice(R, R + 16))
        a, b = rdl[e, side, data, :].astype(F32), rdr[e, side, data, :].astype(F32)
        center = jnp.where(xb, center_of(rdl[e, side, tile, :]), center_of(rdr[e, side, tile, :]))
        if side == 0:
            a, b = pltpu.roll(a, C, 1), pltpu.roll(b, L - C, 1)
        return own, own_center, jnp.where(xb, a, b), center

    END = (0, Y + 1)

    def each_halo(e, use_halo, use_own):
        def body(c, carry):
            found, center = halo_rows(e, c)
            for k, value in enumerate(found):
                use_halo(row_of(c * CH + k + 1), value, center, keep_h)
            return carry

        lax.fori_loop(0, NCH, body, 0)
        each_end(e, use_halo, use_own)

    def each_end(e, use_halo, use_own):
        for side in range(2):
            own, own_center, value, center = end_rows(e, side)
            use_own(END[side] * R, own, own_center, keep_o[side])
            use_halo(END[side] * R, value, center, keep_ho[side])

    def stats_copy(r, k):
        other = lax.rem(me + k, n)
        return pltpu.make_async_remote_copy(
            src_ref=msg.at[r], dst_ref=st.at[r, me],
            send_sem=ss_sem.at[r % 2, k], recv_sem=sr_sem.at[r % 2, me],
            device_id=coords(other), device_id_type=MESH,
        )

    def stats_send(r, top, low):
        row = lax.broadcasted_iota(jnp.int32, (2, L), 0)
        both = jnp.where(row == 0, top, low)
        msg[r] = both
        st[r, me] = both

        def body(k, carry):
            stats_copy(r, k).start()
            return carry

        lax.fori_loop(1, n, body, 0)

    def stats_wait(r):
        def body(k, carry):
            other = lax.rem(me + k, n)
            pltpu.make_async_remote_copy(
                src_ref=msg.at[r], dst_ref=st.at[r, other],
                send_sem=ss_sem.at[r % 2, k], recv_sem=sr_sem.at[r % 2, other],
                device_id=coords(other), device_id_type=MESH,
            ).wait()
            return carry

        lax.fori_loop(1, n, body, 0)
        return jnp.sum(st[r], axis=0)

    def piece_copy(w, phase, k, other, source):
        src = pk.at[w, other] if phase == 0 else ags.at[w]
        dst = (rsb if phase == 0 else agb).at[w, source]
        return pltpu.make_async_remote_copy(
            src_ref=src, dst_ref=dst,
            send_sem=ws_sem.at[w, phase, k], recv_sem=wr_sem.at[w, phase, source],
            device_id=coords(other), device_id_type=MESH,
        )

    def pieces_send(w, phase):
        def body(k, carry):
            piece_copy(w, phase, k, lax.rem(me + k, n), me).start()
            return carry

        lax.fori_loop(1, n, body, 0)

    def pieces_wait(w, phase):
        def body(k, carry):
            other = lax.rem(me + k, n)
            piece_copy(w, phase, k, other, other).wait()
            return carry

        lax.fori_loop(1, n, body, 0)

    def kernel_terms(w, vt, vo, vh):
        for j in range(3):
            g = jnp.concatenate([vo[j * R : (j + Y) * R, :], vh[j * R : (j + Y) * R, :]], axis=1)
            raw[j] = jnp.dot(vt[...], g, preferred_element_type=F32)
        block = lax.broadcasted_iota(jnp.int32, (C, L), 1) // C
        rows_v = cols_a + cols_b
        groups = [jnp.zeros((C, L), F32) for _ in range(7)]
        for j in range(3):
            dy = 2 - j
            for dx in range(3):
                for dz in range(3):
                    tap = dx * 9 + dy * 3 + dz
                    group, slot = tap // 4, tap % 4
                    for kb, (xv, zv) in enumerate(rows_v):
                        for cb, (xg, zg) in enumerate(rows_in):
                            if kb >= 4 and zv == 2 and zg != 1:
                                continue
                            if kb >= 4 and zv == -1 and zg != 0:
                                continue
                            if xv - xg + 1 != dx or zv - zg + 1 != dz:
                                continue
                            t, b = cb // 4, cb % 4
                            part = raw[j, kb * C : (kb + 1) * C, t * L : (t + 1) * L]
                            if slot != b:
                                part = pltpu.roll(part, (slot - b) % 4 * C, 1)
                            groups[group] = groups[group] + jnp.where(block == slot, part, 0.0)
        flat = jnp.concatenate(groups, axis=0)
        rows = n * PIECE
        if rows > flat.shape[0]:
            flat = jnp.concatenate([flat, jnp.zeros((rows - flat.shape[0], L), F32)], axis=0)
        pk[w] = flat.reshape(n, PIECE, L)
        rsb[w, me] = pk[w, me]
        pieces_send(w, 0)

    def pieces_sum(w):
        pieces_wait(w, 0)
        whole = jnp.sum(rsb[w], axis=0)
        ags[w] = whole
        agb[w, me] = whole
        pieces_send(w, 1)

    def pieces_out(w, out_ref, scale):
        pieces_wait(w, 1)
        flat = agb[w].reshape(n * PIECE, L)
        for group in range(7):
            tall = jnp.transpose(flat[group * C : (group + 1) * C]) * scale
            for slot in range(4):
                tap = 4 * group + slot
                if tap < 27:
                    out_ref[tap] = tall[slot * C : (slot + 1) * C]

    def conv_rows(vo, vh, w_ref, c):
        parts = []
        for j in range(3):
            rows = pl.ds(row_of(c * CH + j), CR)
            parts += [vo[rows, :], vh[rows, :]]
        ab = jnp.dot(
            jnp.concatenate(parts, axis=1), w_ref[...].reshape(6 * L, 2 * L),
            preferred_element_type=F32,
        )
        for k in range(CH):
            bs[k, 8 : 8 + R, :] = ab[k * R : (k + 1) * R, L:]
        return [
            ab[k * R : (k + 1) * R, :L]
            + jnp.where(z0, bs[k, 7 : 7 + R, :], bs[k, 9 : 9 + R, :])
            for k in range(CH)
        ]

    def centered(vs):
        s = fold(one(functools.reduce(jnp.add, [eight(v) for v in vs])))
        mean = s / (4.0 * CR)
        high = mean.astype(BF16).astype(F32)
        low = (mean - high).astype(BF16).astype(F32)
        tile = jnp.concatenate(
            [jnp.broadcast_to(high, (8, L)), jnp.broadcast_to(low, (8, L))], axis=0
        )
        return s, high + low, tile

    cells = float(X * Y * Z)
    zero8 = jnp.zeros((8, L), F32)

    def forward_loop(vo, vh, w_ref, hc, centers, e, before):
        def body(c, squares):
            before(c)
            hs = conv_rows(vo, vh, w_ref, c)
            s, center, tile = centered(hs)
            centers[pl.ds(c, 1), :] = center
            scs[pl.ds(c, 1), :] = s
            hs = [h - center for h in hs]
            for k in range(CH):
                hc[pl.ds(row_of(c * CH + k), R), :] = hs[k]
                squares = squares + eight(hs[k] * hs[k])
            pack(e, c, hs, tile)
            send(e, c)
            return squares

        squares = fold(one(lax.fori_loop(0, NCH, body, zero8)))
        mean = one(scs[...]) / cells
        off = centers[...] - mean
        rest = scs[...] - (4.0 * CR) * centers[...]
        spread = squares + one(off * (2.0 * rest + (4.0 * CR) * off))
        return mean, spread

    def moments(r):
        sums = stats_wait(r)
        center = sums[0:1] / n

        def body(d, acc):
            off = st[r, d] - center
            return acc + off * off

        between = lax.fori_loop(0, n, body, jnp.zeros((2, L), F32))[0:1]
        variance = (sums[1:2] + cells * between) / total
        return center, lax.rsqrt(variance + EPSILON)

    build(k1_ref, wf1, True)
    enter(f_ref, vo_f, FEAT)
    pl.semaphore_wait(barrier, n - 1)
    send_all(FEAT)
    build(k2_ref, wf2, True)
    enter(c_ref, vo_c, COT)
    flip(vo_f, vt_f)

    def put_f(dst):
        def use(row, value, center, keep):
            dst[pl.ds(row, R), :] = jnp.where(keep, value, 0.0).astype(BF16)

        return use

    arrive_ends(FEAT)
    each_end(FEAT, put_f(vh_f), put_f(vo_f))

    def take_f(c):
        arrive(side_copies(FEAT, c))
        found, _ = halo_rows(FEAT, c)
        for k, value in enumerate(found):
            put_f(vh_f)(row_of(c * CH + k + 1), value, None, keep_h)

    take_f(0)

    def before_f(c):
        @pl.when(c < NCH - 1)
        def _():
            take_f(c + 1)

    mean, spread = forward_loop(vo_f, vh_f, wf1, hc1, mcs1, HID1, before_f)
    stats_send(0, mean, spread)
    build(k2_ref, wb2, False)
    build(k1_ref, wb1, False)
    center, inv1 = moments(0)
    arrive_all(HID1)
    send_all(COT)

    def put_a(n_dst, v_dst, inv, gain, bias, center):
        def use(row, value, mid, keep):
            normed = (value + (mid - center)) * inv
            n_dst[pl.ds(row, R), :] = normed
            a = activate(normed * gain + bias)
            v_dst[pl.ds(row, R), :] = (a if keep is None else jnp.where(keep, a, 0.0)).astype(BF16)

        return use

    own_a = put_a(n1o, vo_a, inv1, gain1, bias1, center)

    def own_active(c, carry):
        mid = mcs1[pl.ds(c, 1), :]
        for k in range(CH):
            own_a(row_of(c * CH + k + 1), hc1[pl.ds(row_of(c * CH + k), R), :], mid, None)
        return carry

    lax.fori_loop(0, NCH, own_active, 0)
    each_halo(HID1, put_a(n1h, vh_a, inv1, gain1, bias1, center), own_a)

    mean, spread = forward_loop(vo_a, vh_a, wf2, hc2, mcs, HID2, lambda c: None)
    stats_send(1, mean, spread)
    flip(vo_a, vt_a)
    center, inv2 = moments(1)

    def own_output(c, carry):
        plain, along = carry
        mid = mcs[pl.ds(c, 1), :]
        for k in range(CH):
            y = c * CH + k
            normed = (hc2[pl.ds(row_of(y), R), :] + (mid - center)) * inv2
            shifted = normed * gain2 + bias2
            outb[pl.ds(row_of(y), R), :] = activate(shifted).astype(BF16)
            rows = pl.ds(row_of(y + 1), R)
            slope = vo_c[rows, :].astype(F32) * activate_slope(shifted)
            n2o[rows, :] = normed
            s2o[rows, :] = slope
            plain = plain + eight(slope)
            along = along + eight(slope * normed)
        return plain, along

    plain, along = lax.fori_loop(0, NCH, own_output, (zero8, zero8))
    stats_send(2, fold(one(plain)), fold(one(along)))

    arrive_all(COT)
    arrive_all(HID2)

    def put_c(dst):
        def use(row, value, mid, keep):
            dst[pl.ds(row, R), :] = value.astype(BF16)

        return use

    each_halo(COT, put_c(vh_c), put_c(vo_c))

    def put_s(n_dst, s_dst, c_src):
        def use(row, value, mid, keep):
            rows = pl.ds(row, R)
            normed = (value + (mid - center)) * inv2
            n_dst[rows, :] = normed
            s_dst[rows, :] = c_src[rows, :].astype(F32) * activate_slope(normed * gain2 + bias2)

        return use

    each_halo(HID2, put_s(n2h, s2h, vh_c), put_s(n2o, s2o, vo_c))
    leave(outb, o_ref)
    sums2 = stats_wait(2)

    def gradient(slope, normed, sums, factor):
        return factor * (slope - sums[0:1] / total - normed * (sums[1:2] / total))

    factor2 = gain2 * inv2

    def grad_rows(row, keep_own, keep_halo):
        rows = pl.ds(row, R)
        g = gradient(s2o[rows, :], n2o[rows, :], sums2, factor2)
        vo_g[rows, :] = (g if keep_own is None else jnp.where(keep_own, g, 0.0)).astype(BF16)
        g = gradient(s2h[rows, :], n2h[rows, :], sums2, factor2)
        vh_g[rows, :] = jnp.where(keep_halo, g, 0.0).astype(BF16)

    def grad_two(c, carry):
        for k in range(CH):
            grad_rows(row_of(c * CH + k + 1), None, keep_h)
        return carry

    lax.fori_loop(0, NCH, grad_two, 0)
    for side in range(2):
        grad_rows(END[side] * R, keep_o[side], keep_ho[side])

    def back_loop(c, carry):
        plain, along = carry
        slopes = []
        for k, back in enumerate(conv_rows(vo_g, vh_g, wb2, c)):
            rows = pl.ds(row_of(c * CH + k + 1), R)
            normed = n1o[rows, :]
            slope = back * activate_slope(normed * gain1 + bias1)
            s1o[rows, :] = slope
            plain = plain + eight(slope)
            along = along + eight(slope * normed)
            slopes.append(slope)
        _, mid, tile = centered(slopes)
        pack(SLO1, c, [v - mid for v in slopes], tile)
        send(SLO1, c)
        return plain, along

    plain, along = lax.fori_loop(0, NCH, back_loop, (zero8, zero8))
    stats_send(3, fold(one(plain)), fold(one(along)))
    kernel_terms(1, vt_a, vo_g, vh_g)
    sums1 = stats_wait(3)
    arrive_all(SLO1)
    factor1 = gain1 * inv1

    def put_g(dst, normed_ref):
        def use(row, value, mid, keep):
            rows = pl.ds(row, R)
            g = gradient(value + mid, normed_ref[rows, :], sums1, factor1)
            dst[rows, :] = jnp.where(keep, g, 0.0).astype(BF16)

        return use

    def grad_one(c, carry):
        for k in range(CH):
            rows = pl.ds(row_of(c * CH + k + 1), R)
            vo_g[rows, :] = gradient(s1o[rows, :], n1o[rows, :], sums1, factor1).astype(BF16)
        return carry

    lax.fori_loop(0, NCH, grad_one, 0)
    each_halo(SLO1, put_g(vh_g, n1h), put_g(vo_g, n1o))
    kernel_terms(0, vt_f, vo_g, vh_g)
    pieces_sum(1)

    def last_loop(c, carry):
        for k, back in enumerate(conv_rows(vo_g, vh_g, wb1, c)):
            outb[pl.ds(row_of(c * CH + k), R), :] = back.astype(BF16)
        return carry

    lax.fori_loop(0, NCH, last_loop, 0)
    pieces_sum(0)
    leave(outb, fg_ref)
    scale = 1.0 / (total ** 0.5)
    for row, (sums, part) in enumerate(((sums1, 1), (sums1, 0), (sums2, 1), (sums2, 0))):
        ng_ref[row : row + 1, :] = sums[part : part + 1, 0:C] * scale
    pieces_out(1, dk2_ref, scale)
    pieces_out(0, dk1_ref, scale)
    for e in range(NEXCH):
        sent_all(e)


def local(features, kernel_one, gain_one, bias_one, kernel_two, gain_two, bias_two, cotangent):
    C, X, Y, Z = features.shape
    nx, ny = lax.axis_size("gx"), lax.axis_size("gy")
    n = nx * ny
    total = float(X * Y * Z * nx * ny)
    R = Z // 2
    NCH = Y // CH
    piece = -(-224 // (8 * n)) * 8
    taps = lambda k: jnp.transpose(k, (2, 3, 4, 0, 1)).reshape(27, C, C)
    row = lambda v: v.reshape(1, C)
    rows, all_rows = Y * R, (Y + 2) * R
    packed = CH * R // 2 + 16
    V = pltpu.VMEM
    DMA = pltpu.SemaphoreType.DMA
    scratch = [
        V((rows, L), F32), V((8, L), F32), V((R, 2 * Z), BF16), V((2 * L, 2 * Z), BF16),
        V((L, L), BF16), V((27, C, L), F32),
    ]
    scratch += [V((3, 2 * L, 2 * L), BF16)] * 4
    scratch += [V((all_rows, L), BF16)] * 8
    scratch += [V((2 * L, rows), BF16)] * 2
    scratch += [V((rows, L), F32)] * 2
    scratch += [V((all_rows, L), F32)] * 7
    scratch += [
        V((rows, L), BF16), V((CH, R + 16, L), F32), V((NCH, L), F32), V((NCH, L), F32),
        V((NCH, L), F32), V((3, 2 * L, 2 * L), F32),
    ]
    scratch += [V((NEXCH, NCH, packed, L), BF16)] * 2 + [V((NEXCH, 2, R + 16, L), BF16)]
    scratch += [V((NEXCH, NCH, packed, L), BF16)] * 2 + [V((NEXCH, 2, R + 16, L), BF16)] * 3
    scratch += [DMA((NEXCH, 2 * NCH + 6))] * 2
    scratch += [V((4, 2, L), F32), V((4, n, 2, L), F32), DMA((2, n)), DMA((2, n))]
    scratch += [
        V((2, n, piece, L), F32), V((2, n, piece, L), F32), V((2, piece, L), F32),
        V((2, n, piece, L), F32), DMA((2, 2, n)), DMA((2, 2, n)),
    ]
    vmem = pl.BlockSpec(memory_space=pltpu.VMEM)
    out, fg, dk1, dk2, norm = pl.pallas_call(
        functools.partial(kernel, nx, ny, total),
        name="blocks",
        out_shape=[
            jax.ShapeDtypeStruct((C, X, Y, Z), BF16), jax.ShapeDtypeStruct((C, X, Y, Z), BF16),
            jax.ShapeDtypeStruct((27, C, C), F32), jax.ShapeDtypeStruct((27, C, C), F32),
            jax.ShapeDtypeStruct((4, C), F32),
        ],
        in_specs=[vmem] * 8,
        out_specs=[vmem] * 5,
        scratch_shapes=scratch,
        compiler_params=pltpu.CompilerParams(
            collective_id=0, has_side_effects=True, vmem_limit_bytes=62 << 20
        ),
    )(
        features, cotangent, taps(kernel_one), taps(kernel_two),
        row(gain_one), row(bias_one), row(gain_two), row(bias_two),
    )
    untap = lambda d: jnp.transpose(d.reshape(3, 3, 3, C, C), (3, 4, 0, 1, 2))
    return out, fg, untap(dk1), untap(dk2), norm


def solution(mesh):
    in_specs = (P(None, "gx", "gy", None), P(), P(), P(), P(), P(), P(), P(None, "gx", "gy", None))
    out_specs = (P(None, "gx", "gy", None), P(None, "gx", "gy", None), P(), P(), P())
    return jax.shard_map(local, mesh=mesh, in_specs=in_specs, out_specs=out_specs, check_vma=False)
```

```python
import functools

import jax
import jax.numpy as jnp
from jax import lax
from jax.experimental import pallas as pl
from jax.experimental.pallas import tpu as pltpu
from jax.sharding import PartitionSpec as P

EPSILON = 1e-05
SLOPE = 0.01
SHARPNESS = 8.0
MESH = pl.DeviceIdType.MESH
LOGICAL = pl.DeviceIdType.LOGICAL
F32 = jnp.float32
BF16 = jnp.bfloat16
L = 128
CH = 4
FEAT, COT, HID1, HID2, SLO1 = range(5)
NEXCH = 5
NT = (((1,), (1,)), ((), ()))


def activate(s):
    scaled = SHARPNESS * s
    soft = jnp.maximum(scaled, 0.0) + jnp.log(1.0 + jnp.exp(-jnp.abs(scaled)))
    return SLOPE * s + ((1.0 - SLOPE) / SHARPNESS) * soft


def activate_slope(s):
    half = 0.5 * (1.0 - SLOPE)
    return (SLOPE + half) + half * jnp.tanh((0.5 * SHARPNESS) * s)


def kernel(
    nx, ny, total,
    f_hbm, c_hbm, k1_hbm, k2_hbm, g1_hbm, b1_hbm, g2_hbm, b2_hbm,
    o_ref, fg_ref, dk_ref, ng_ref,
    t1, par, e_mat, s_mat, i_mat, base, wf1, wf2, wb2, wb1,
    vo_f, vh_f, vo_c, vh_c, vo_a, vh_a, vo_g, vh_g, vt_f, vt_a,
    hc1, hc2, n1o, n1h, n2o, n2h, s2o, s2h, s1o, outb, bs, mcs, scs, mcs1, raw,
    spr, spl, se, rl, rr, re, rdl, rdr, hs_sem, hr_sem,
    msg, st, ss_sem, sr_sem,
    pk, rsb, ags, agb, ws_sem, wr_sem,
    f_ref, c_ref, k1_ref, k2_ref, g1_ref, b1_ref, g2_ref, b2_ref, in_sem, rel, rel_sem, fwd_sem,
):
    C, X, Y, Z = f_ref.shape
    R = Z // 2
    CR = CH * R
    NCH = Y // CH
    n = nx * ny
    PIECE = rsb.shape[2]
    gx, gy = lax.axis_index("gx"), lax.axis_index("gy")
    me = gx * ny + gy
    has_l, has_r = gx > 0, gx < nx - 1
    has_d, has_u = gy > 0, gy < ny - 1

    def peer(k):
        other = me + k
        return jnp.where(other >= n, other - n, other)

    fetch = [
        pltpu.make_async_copy(src, dst, in_sem.at[k])
        for k, (src, dst) in enumerate(
            (
                (k1_hbm, k1_ref), (f_hbm, f_ref), (k2_hbm, k2_ref), (c_hbm, c_ref),
                (g1_hbm, g1_ref), (b1_hbm, b1_ref), (g2_hbm, g2_ref), (b2_hbm, b2_ref),
            )
        )
    ]
    for copy in fetch:
        copy.start()

    barrier = pltpu.get_barrier_semaphore()

    def hello(k, carry):
        pl.semaphore_signal(barrier, inc=1, device_id=peer(k), device_id_type=LOGICAL)
        return carry

    lax.fori_loop(1, n, hello, 0)

    lane = lax.broadcasted_iota(jnp.int32, (1, L), 1)
    xb = lax.rem(lane // C, 2) == 1
    z0 = lane < L // 2
    flag = lambda b: jnp.where(b, 1, 0)
    keep_h = jnp.where(xb, flag(has_l), flag(has_r)) > 0
    full_y = jnp.full((1, L), 1, jnp.int32)
    keep_o = [full_y * flag(has_d) > 0, full_y * flag(has_u) > 0]
    keep_ho = [(jnp.where(xb, flag(has_l), flag(has_r)) * flag(b)) > 0 for b in (has_d, has_u)]

    def row_of(y):
        return pl.multiple_of(y * R, R)

    def fold(v):
        v = v + pltpu.roll(v, C, 1)
        return v + pltpu.roll(v, 2 * C, 1)

    def loop(count, body, carry=0, unroll=1):
        def group(i, carry):
            for k in range(unroll):
                carry = body(i * unroll + k, carry)
            return carry

        return lax.fori_loop(0, count // unroll, group, carry)

    def eight(v):
        return jnp.sum(v.reshape(v.shape[0] // 8, 8, L), axis=0)

    def one(v):
        return jnp.sum(v, axis=0, keepdims=True)

    r_i = lax.broadcasted_iota(jnp.int32, (R, 2 * Z), 0)
    c_i = lax.broadcasted_iota(jnp.int32, (R, 2 * Z), 1)
    e_mat[...] = jnp.where(
        lax.rem(c_i, Z) == 2 * r_i + c_i // Z, 1.0, 0.0
    ).astype(BF16)
    r_i = lax.broadcasted_iota(jnp.int32, (2 * L, 2 * Z), 0)
    c_i = lax.broadcasted_iota(jnp.int32, (2 * L, 2 * Z), 1)
    same = lax.rem(r_i // R, 2) == c_i // Z
    s_mat[...] = jnp.where(
        same & (lax.rem(c_i, Z) == 2 * lax.rem(r_i, R) + r_i // L), 1.0, 0.0
    ).astype(BF16)
    r_i = lax.broadcasted_iota(jnp.int32, (L, L), 0)
    c_i = lax.broadcasted_iota(jnp.int32, (L, L), 1)
    i_mat[...] = jnp.where(r_i == c_i, 1.0, 0.0).astype(BF16)
    bs[...] = jnp.zeros(bs.shape, F32)

    spots_in = [(0, 0, z, x) for z in range(2) for x in range(2)]
    halo_x = {0: 2, 1: -1}
    rows_in = [(x, z) for _, _, z, x in spots_in] + [(halo_x[x], z) for _, _, z, x in spots_in]
    cols_a = [(x, z) for _, _, z, x in spots_in]
    cols_b = [(x, 2 if z == 0 else -1) for _, _, z, x in spots_in]

    def build(k_ref, w_ref, forward):
        if forward:
            stacked = jnp.concatenate([k_ref[t] for t in range(27) for _ in range(4)], axis=0)
            wide = lax.dot_general(
                i_mat[0:C, 0:C], stacked, NT, preferred_element_type=F32
            )
            for t in range(27):
                base[t] = wide[:, t * L : (t + 1) * L]
        else:
            r4 = lax.broadcasted_iota(jnp.int32, (C, L), 0)
            c4 = lax.rem(lax.broadcasted_iota(jnp.int32, (C, L), 1), C)
            spread4 = jnp.where(r4 == c4, 1.0, 0.0).astype(BF16)
            tall = k_ref[...].reshape(27 * C, C)
            wide = jnp.dot(tall, spread4, preferred_element_type=F32)
            for t in range(27):
                base[t] = wide[t * C : (t + 1) * C]
        block = lax.broadcasted_iota(jnp.int32, (C, L), 1) // C

        def one_row(j, carry):
            dy = j if forward else 2 - j
            for kb, (xi, zi) in enumerate(rows_in):
                for t, cols in enumerate((cols_a, cols_b)):
                    value = jnp.zeros((C, L), F32)
                    for b, (xo, zo) in enumerate(cols):
                        dx, dz = xi - xo + 1, zi - zo + 1
                        if not forward:
                            dx, dz = 2 - dx, 2 - dz
                        if 0 <= dx <= 2 and 0 <= dz <= 2:
                            tap = base[dx * 9 + dy * 3 + dz]
                            value = jnp.where(block == b, tap, value)
                    w_ref[j, kb * C : (kb + 1) * C, t * L : (t + 1) * L] = value.astype(BF16)
            return carry

        lax.fori_loop(0, 3, one_row, 0)

    def enter(in_ref, vo, e):
        def widen(c, carry):
            t1[pl.ds(pl.multiple_of(c * X * Y, X * Y), X * Y), :] = (
                in_ref[c].reshape(X * Y, Z).astype(F32)
            )
            return carry

        loop(C, widen, unroll=4)
        zero = jnp.zeros((X * C, Z), BF16)

        def chunk(c, carry):
            vs = []
            for k in range(CH):
                y = c * CH + k
                x0 = t1[pl.ds(y, C, stride=X * Y), :]
                x1 = t1[pl.ds(Y + y, C, stride=X * Y), :]
                xy = jnp.concatenate([x0, x1], axis=0).astype(BF16)
                rhs = jnp.concatenate(
                    [jnp.concatenate([xy, zero], axis=1), jnp.concatenate([zero, xy], axis=1)],
                    axis=0,
                )
                v = lax.dot_general(e_mat[...], rhs, NT, preferred_element_type=F32)
                vo[pl.ds(row_of(y + 1), R), :] = v.astype(BF16)
                vs.append(v)
            pack(e, c, vs, None)
            return carry

        loop(NCH, chunk, unroll=2)

    def leave(src, dst):
        def pair(p, carry):
            o = src[pl.ds(pl.multiple_of(p * L, L), L), :]
            d = lax.dot_general(i_mat[...], o, NT, preferred_element_type=F32).astype(BF16)
            both = jnp.concatenate([d[: L // 2], d[L // 2 :]], axis=1)
            xs = jnp.dot(both, s_mat[...], preferred_element_type=F32)
            r0 = pl.multiple_of(p * 2 * R, 2 * R)
            t1[pl.ds(r0, R), :] = xs[:, :Z]
            t1[pl.ds(r0 + R, R), :] = xs[:, Z:]
            return carry

        with jax.named_scope("leave_pairs"):
            loop(Y // 2, pair, unroll=4)

        def channel(c, carry):
            for x in range(X):
                dst[c, x] = t1[pl.ds(x * C + c, Y, stride=X * C), :].astype(BF16)
            return carry

        with jax.named_scope("leave_channels"):
            loop(C, channel, unroll=4)

    def flip(vo, vt):
        def pair(p, carry):
            rows = vo[pl.ds(row_of(2 * p + 1), 2 * R), :]
            wide = rows.astype(F32)
            slot = 2 * lax.rem(p, 4)
            for k in range(2):
                bs[slot + k, 8 : 8 + R, :] = wide[k * R : (k + 1) * R]
            shifted = jnp.concatenate(
                [jnp.where(z0, bs[slot + k, 9 : 9 + R, :], bs[slot + k, 7 : 7 + R, :]) for k in range(2)],
                axis=0,
            ).astype(BF16)
            cols = pl.ds(pl.multiple_of(p * 2 * R, 2 * R), 2 * R)
            for k, part in enumerate((rows, shifted)):
                vt[k * L : (k + 1) * L, cols] = lax.dot_general(
                    i_mat[...], part, NT, preferred_element_type=F32
                ).astype(BF16)
            return carry

        loop(Y // 2, pair, unroll=4)

    half = CR // 2

    def pack(e, c, vs, center):
        for p in range(CH // 2):
            a, b = vs[2 * p], vs[2 * p + 1]
            rows = slice(p * (R + 16), p * (R + 16) + R)
            spr[e, c, rows, :] = jnp.where(xb, a, pltpu.roll(b, L - C, 1)).astype(BF16)
            spl[e, c, rows, :] = jnp.where(xb, pltpu.roll(b, C, 1), a).astype(BF16)
        if center is not None:
            center = center.astype(BF16)
            spr[e, c, R : R + 16, :] = center
            spl[e, c, R : R + 16, :] = center

        first = jnp.where(c == 0, 0, 2)
        se[e, first, 0:R, :] = vs[0].astype(BF16)
        if center is not None:
            se[e, first, R : R + 16, :] = center
        last = jnp.where(c == NCH - 1, 1, 2)
        se[e, last, 0:R, :] = vs[CH - 1].astype(BF16)
        if center is not None:
            se[e, last, R : R + 16, :] = center

    def copy_of(e, index, src, dst, dx, dy):
        return lambda: pltpu.make_async_remote_copy(
            src_ref=src, dst_ref=dst,
            send_sem=hs_sem.at[e, index], recv_sem=hr_sem.at[e, index],
            device_id=(lax.rem(gx + dx + nx, nx), lax.rem(gy + dy + ny, ny)),
            device_id_type=MESH,
        )

    def side_copies(e, c):
        return [
            (has_r, has_l, copy_of(e, c, spr.at[e, c], rl.at[e, c], 1, 0)),
            (has_l, has_r, copy_of(e, NCH + c, spl.at[e, c], rr.at[e, c], -1, 0)),
        ]

    def end_copies(e):
        low, high = pl.ds(0, R + 16), pl.ds(R, R + 16)
        both = jnp.logical_and
        m = 2 * NCH
        last = NCH - 1
        return [
            [
                (has_d, has_u, copy_of(e, m, se.at[e, 0], re.at[e, 1], 0, -1)),
                (both(has_r, has_d), both(has_l, has_u),
                 copy_of(e, m + 2, spr.at[e, 0, low], rdl.at[e, 1], 1, -1)),
                (both(has_l, has_d), both(has_r, has_u),
                 copy_of(e, m + 4, spl.at[e, 0, low], rdr.at[e, 1], -1, -1)),
            ],
            [
                (has_u, has_d, copy_of(e, m + 1, se.at[e, 1], re.at[e, 0], 0, 1)),
                (both(has_r, has_u), both(has_l, has_d),
                 copy_of(e, m + 3, spr.at[e, last, high], rdl.at[e, 0], 1, 1)),
                (both(has_l, has_u), both(has_r, has_d),
                 copy_of(e, m + 5, spl.at[e, last, high], rdr.at[e, 0], -1, 1)),
            ],
        ]

    def start(copies):
        for sends, _, copy in copies:
            @pl.when(sends)
            def _(copy=copy):
                copy().start()

    def arrive(copies):
        for _, takes, copy in copies:
            @pl.when(takes)
            def _(copy=copy):
                copy().wait_recv()

    RELAY = nx == 8
    ODD = range(NCH // 2)
    low_mid, high_mid = nx // 2 - 1, nx // 2

    def hop(e, h, src, dst, there, s_sem, r_sem):
        return pltpu.make_async_remote_copy(
            src_ref=src, dst_ref=dst, send_sem=s_sem, recv_sem=r_sem,
            device_id=(there, gy), device_id_type=MESH,
        )

    def send_odd(e, c):
        h = c // 2
        (_, _, right), (_, _, left) = side_copies(e, c)
        relays = (
            (gx == low_mid, has_r, right, spr, nx - 1, hs_sem.at[e, c]),
            (gx == high_mid, has_l, left, spl, 0, hs_sem.at[e, NCH + c]),
        )
        for via, sends, direct, src, there, s_sem in relays:
            @pl.when(via)
            def _(src=src, there=there, s_sem=s_sem):
                hop(e, h, src.at[e, c], rel.at[e, h], there, s_sem, rel_sem.at[e, h]).start()

            @pl.when(jnp.logical_and(sends, jnp.logical_not(via)))
            def _(direct=direct):
                direct().start()

    def forwards(e, h):
        c = 2 * h + 1
        return (
            (gx == nx - 1, hop(e, h, rel.at[e, h], rl.at[e, c], high_mid, fwd_sem.at[e, h], hr_sem.at[e, c])),
            (gx == 0, hop(e, h, rel.at[e, h], rr.at[e, c], low_mid, fwd_sem.at[e, h], hr_sem.at[e, NCH + c])),
        ) if RELAY else ()

    def relay_arrives(e, h):
        hop(e, h, rel.at[e, h], rel.at[e, h], low_mid, fwd_sem.at[e, h], rel_sem.at[e, h]).wait_recv()

    def forward(e, which):
        for h in which:
            for here, copy in forwards(e, h):
                @pl.when(here)
                def _(h=h, copy=copy):
                    relay_arrives(e, h)
                    copy.start()

    def forwarded(e):
        for h in ODD:
            for here, copy in forwards(e, h):
                @pl.when(here)
                def _(copy=copy):
                    copy.wait_send()

    def send(e, c, odd):
        if RELAY and odd:
            send_odd(e, c)
        else:
            start(side_copies(e, c))

    def send_ends(e):
        for copies in end_copies(e):
            start(copies)

    def send_all(e):
        def body(h, carry):
            send(e, 2 * h, False)
            send(e, 2 * h + 1, True)
            return carry

        lax.fori_loop(0, NCH // 2, body, 0)
        send_ends(e)

    def arrive_ends(e):
        for copies in end_copies(e):
            arrive(copies)

    def arrive_all(e):
        def body(c, carry):
            arrive(side_copies(e, c))
            return carry

        lax.fori_loop(0, NCH, body, 0)
        arrive_ends(e)

    def sent_all(e):
        def done(copies):
            for sends, _, copy in copies:
                @pl.when(sends)
                def _(copy=copy):
                    copy().wait_send()

        def body(c, carry):
            done(side_copies(e, c))
            return carry

        lax.fori_loop(0, NCH, body, 0)
        for copies in end_copies(e):
            done(copies)

    def center_of(tile):
        wide = tile.astype(F32)
        return (wide[0:8] + wide[8:16])[0:1]

    def halo_rows(e, c):
        center = jnp.where(xb, center_of(rl[e, c, R : R + 16, :]), center_of(rr[e, c, R : R + 16, :]))
        found = []
        for p in range(CH // 2):
            rows = slice(p * (R + 16), p * (R + 16) + R)
            a, b = rl[e, c, rows, :].astype(F32), rr[e, c, rows, :].astype(F32)
            found.append(jnp.where(xb, a, b))
            found.append(jnp.where(xb, pltpu.roll(a, C, 1), pltpu.roll(b, L - C, 1)))
        return found, center

    def end_rows(e, side):
        own, own_center = re[e, side, 0:R, :].astype(F32), center_of(re[e, side, R : R + 16, :])
        data, tile = (slice(16, 16 + R), slice(0, 16)) if side == 0 else (slice(0, R), slice(R, R + 16))
        a, b = rdl[e, side, data, :].astype(F32), rdr[e, side, data, :].astype(F32)
        center = jnp.where(xb, center_of(rdl[e, side, tile, :]), center_of(rdr[e, side, tile, :]))
        if side == 0:
            a, b = pltpu.roll(a, C, 1), pltpu.roll(b, L - C, 1)
        return own, own_center, jnp.where(xb, a, b), center

    END = (0, Y + 1)

    def each_halo(e, use_halo, use_own):
        def body(c, carry):
            found, center = halo_rows(e, c)
            for k, value in enumerate(found):
                use_halo(row_of(c * CH + k + 1), value, center, keep_h)
            return carry

        lax.fori_loop(0, NCH, body, 0)
        each_end(e, use_halo, use_own)

    def each_end(e, use_halo, use_own):
        for side in range(2):
            own, own_center, value, center = end_rows(e, side)
            use_own(END[side] * R, own, own_center, keep_o[side])
            use_halo(END[side] * R, value, center, keep_ho[side])

    def stats_send(r, top, low):
        row = lax.broadcasted_iota(jnp.int32, (2, L), 0)
        both = jnp.where(row == 0, top, low)
        msg[r] = both
        st[r, me] = both

        def body(k, carry):
            pltpu.make_async_remote_copy(
                src_ref=msg.at[r], dst_ref=st.at[r, me],
                send_sem=ss_sem.at[r], recv_sem=sr_sem.at[r],
                device_id=peer(k), device_id_type=LOGICAL,
            ).start()
            return carry

        lax.fori_loop(1, n, body, 0)

    def stats_wait(r):
        others = st.at[r, pl.ds(0, n - 1)]
        pltpu.make_async_remote_copy(
            src_ref=others, dst_ref=others, send_sem=ss_sem.at[r], recv_sem=sr_sem.at[r],
            device_id=peer(1), device_id_type=LOGICAL,
        ).wait()
        return jnp.sum(st[r], axis=0)

    def pieces_send(w, phase):
        def body(k, carry):
            other = peer(k)
            pltpu.make_async_remote_copy(
                src_ref=pk.at[w, other] if phase == 0 else ags.at[w],
                dst_ref=(rsb if phase == 0 else agb).at[w, me],
                send_sem=ws_sem.at[w, phase], recv_sem=wr_sem.at[w, phase],
                device_id=other, device_id_type=LOGICAL,
            ).start()
            return carry

        lax.fori_loop(1, n, body, 0)

    def pieces_wait(w, phase):
        others = (rsb if phase == 0 else agb).at[w, pl.ds(0, n - 1)]
        pltpu.make_async_remote_copy(
            src_ref=others, dst_ref=others,
            send_sem=ws_sem.at[w, phase], recv_sem=wr_sem.at[w, phase],
            device_id=peer(1), device_id_type=LOGICAL,
        ).wait()

    def kernel_terms(w, vt, vo, vh):
        for j in range(3):
            g = jnp.concatenate([vo[j * R : (j + Y) * R, :], vh[j * R : (j + Y) * R, :]], axis=1)
            raw[j] = jnp.dot(vt[...], g, preferred_element_type=F32)
        block = lax.broadcasted_iota(jnp.int32, (C, L), 1) // C
        rows_v = cols_a + cols_b
        groups = [jnp.zeros((C, L), F32) for _ in range(7)]
        for j in range(3):
            dy = 2 - j
            for dx in range(3):
                for dz in range(3):
                    tap = dx * 9 + dy * 3 + dz
                    group, slot = tap // 4, tap % 4
                    for kb, (xv, zv) in enumerate(rows_v):
                        for cb, (xg, zg) in enumerate(rows_in):
                            if kb >= 4 and zv == 2 and zg != 1:
                                continue
                            if kb >= 4 and zv == -1 and zg != 0:
                                continue
                            if xv - xg + 1 != dx or zv - zg + 1 != dz:
                                continue
                            t, b = cb // 4, cb % 4
                            part = raw[j, kb * C : (kb + 1) * C, t * L : (t + 1) * L]
                            if slot != b:
                                part = pltpu.roll(part, (slot - b) % 4 * C, 1)
                            groups[group] = groups[group] + jnp.where(block == slot, part, 0.0)
        flat = jnp.concatenate(groups, axis=0)
        rows = n * PIECE
        if rows > flat.shape[0]:
            flat = jnp.concatenate([flat, jnp.zeros((rows - flat.shape[0], L), F32)], axis=0)
        pk[w] = flat.reshape(n, PIECE, L)
        rsb[w, me] = pk[w, me]
        pieces_send(w, 0)

    def pieces_sum(w):
        pieces_wait(w, 0)
        whole = jnp.sum(rsb[w], axis=0).astype(BF16)
        ags[w] = whole
        agb[w, me] = whole
        pieces_send(w, 1)

    def pieces_out(w):
        pieces_wait(w, 1)
        dk_ref[w] = agb[w].reshape(n * PIECE, L)

    def conv_rows(vo, vh, w_ref, c, slot=0):
        parts = []
        for j in range(3):
            rows = pl.ds(row_of(c * CH + j), CR)
            parts += [vo[rows, :], vh[rows, :]]
        ab = jnp.dot(
            jnp.concatenate(parts, axis=1), w_ref[...].reshape(6 * L, 2 * L),
            preferred_element_type=F32,
        )
        for k in range(CH):
            bs[slot + k, 8 : 8 + R, :] = ab[k * R : (k + 1) * R, L:]
        return [
            ab[k * R : (k + 1) * R, :L]
            + jnp.where(z0, bs[slot + k, 7 : 7 + R, :], bs[slot + k, 9 : 9 + R, :])
            for k in range(CH)
        ]

    def totals(vs):
        return fold(one(functools.reduce(jnp.add, [eight(v) for v in vs])))

    def center_near(s):
        mean = s / (4.0 * CR)
        high = mean.astype(BF16).astype(F32)
        low = (mean - high).astype(BF16).astype(F32)
        tile = jnp.concatenate(
            [jnp.broadcast_to(high, (8, L)), jnp.broadcast_to(low, (8, L))], axis=0
        )
        return high + low, tile

    cells = float(X * Y * Z)
    zero8 = jnp.zeros((8, L), F32)
    PAIR = 2

    def paired(e, step, carry, before=None):
        def group(i, carry, first):
            inner, s = carry
            if before is not None:
                before(i)
            found = []
            for k in range(PAIR):
                inner, vs = step(i * PAIR + k, k * CH, inner)
                found.append((vs, totals(vs)))
            center, tile = center_near(found[0][1] if first else s)
            for k, (vs, s) in enumerate(found):
                c = i * PAIR + k
                centers_of[e][pl.ds(c, 1), :] = center
                scs[pl.ds(c, 1), :] = s
                inner = keep_chunk(e, c, vs, center, tile, inner)
            if e != HID2:
                for k in range(PAIR):
                    send(e, i * PAIR + k, k % 2 == 1)
            return inner, s

        carry = group(0, (carry, None), True)
        carry = lax.fori_loop(1, NCH // PAIR, lambda i, x: group(i, x, False), carry)
        if e != HID2:
            send_ends(e)
        return carry[0]

    centers_of = {HID1: mcs1, HID2: mcs, SLO1: mcs}

    def keep_chunk(e, c, vs, center, tile, inner):
        vs = [v - center for v in vs]
        pack(e, c, vs, tile)
        if e != SLO1:
            hc = hc1 if e == HID1 else hc2
            for k, v in enumerate(vs):
                hc[pl.ds(row_of(c * CH + k), R), :] = v
                inner = inner + eight(v * v)
        return inner

    def forward_loop(vo, vh, w_ref, e, before):
        def step(c, slot, squares):
            return squares, conv_rows(vo, vh, w_ref, c, slot)

        squares = fold(one(paired(e, step, zero8, before)))
        centers = centers_of[e][...]
        mean = one(scs[...]) / cells
        off = centers - mean
        rest = scs[...] - (4.0 * CR) * centers
        spread = squares + one(off * (2.0 * rest + (4.0 * CR) * off))
        return mean, spread

    def moments(r):
        sums = stats_wait(r)
        center = sums[0:1] / n

        def body(d, acc):
            off = st[r, d] - center
            return acc + off * off

        between = lax.fori_loop(0, n, body, jnp.zeros((2, L), F32))[0:1]
        variance = (sums[1:2] + cells * between) / total
        return center, lax.rsqrt(variance + EPSILON)

    fetch[0].wait()
    build(k1_ref, wf1, True)
    fetch[1].wait()
    enter(f_ref, vo_f, FEAT)
    pl.semaphore_wait(barrier, n - 1)
    send_all(FEAT)
    fetch[2].wait()
    build(k2_ref, wf2, True)
    build(k2_ref, wb2, False)
    build(k1_ref, wb1, False)
    fetch[3].wait()
    enter(c_ref, vo_c, COT)
    forward(FEAT, ODD)

    def put_f(dst):
        def use(row, value, center, keep):
            dst[pl.ds(row, R), :] = jnp.where(keep, value, 0.0).astype(BF16)

        return use

    arrive_ends(FEAT)
    each_end(FEAT, put_f(vh_f), put_f(vo_f))

    def take_f(c):
        found, _ = halo_rows(FEAT, c)
        for k, value in enumerate(found):
            put_f(vh_f)(row_of(c * CH + k + 1), value, None, keep_h)

    arrive(side_copies(FEAT, 0))
    take_f(0)

    def before_f(i):
        low = i * PAIR + 1
        high = jnp.minimum(low + 1, NCH - 1)
        arrive(side_copies(FEAT, low))

        @pl.when(high > low)
        def _():
            arrive(side_copies(FEAT, high))

        take_f(low)
        take_f(high)

    mean, spread = forward_loop(vo_f, vh_f, wf1, HID1, before_f)
    stats_send(0, mean, spread)
    for copy in fetch[4:]:
        copy.wait()
    par[...] = jnp.zeros(par.shape, F32)
    for row, ref in enumerate((g1_ref, b1_ref, g2_ref, b2_ref)):
        par[row : row + 1, 0:C] = ref[...]
    params = fold(par[...])
    gain1, bias1, gain2, bias2 = [params[r : r + 1] for r in range(4)]
    forward(HID1, ODD[: NCH // 4])
    flip(vo_f, vt_f)
    forward(HID1, ODD[NCH // 4 :])
    center, inv1 = moments(0)
    arrive_all(HID1)
    send_all(COT)

    def put_a(n_dst, v_dst, inv, gain, bias, center):
        def use(row, value, mid, keep):
            normed = (value + (mid - center)) * inv
            n_dst[pl.ds(row, R), :] = normed
            a = activate(normed * gain + bias)
            v_dst[pl.ds(row, R), :] = (a if keep is None else jnp.where(keep, a, 0.0)).astype(BF16)

        return use

    own_a = put_a(n1o, vo_a, inv1, gain1, bias1, center)

    def own_active(c, carry):
        mid = mcs1[pl.ds(c, 1), :]
        for k in range(CH):
            own_a(row_of(c * CH + k + 1), hc1[pl.ds(row_of(c * CH + k), R), :], mid, None)
        return carry

    lax.fori_loop(0, NCH, own_active, 0)
    each_halo(HID1, put_a(n1h, vh_a, inv1, gain1, bias1, center), own_a)
    forward(COT, ODD)

    mean, spread = forward_loop(vo_a, vh_a, wf2, HID2, None)
    stats_send(1, mean, spread)
    send_all(HID2)
    flip(vo_a, vt_a)
    forward(HID2, ODD)
    center, inv2 = moments(1)

    def own_output(c, carry):
        plain, along = carry
        mid = mcs[pl.ds(c, 1), :]
        for k in range(CH):
            y = c * CH + k
            normed = (hc2[pl.ds(row_of(y), R), :] + (mid - center)) * inv2
            shifted = normed * gain2 + bias2
            outb[pl.ds(row_of(y), R), :] = activate(shifted).astype(BF16)
            rows = pl.ds(row_of(y + 1), R)
            slope = vo_c[rows, :].astype(F32) * activate_slope(shifted)
            n2o[rows, :] = normed
            s2o[rows, :] = slope
            plain = plain + eight(slope)
            along = along + eight(slope * normed)
        return plain, along

    plain, along = lax.fori_loop(0, NCH, own_output, (zero8, zero8))
    stats_send(2, fold(one(plain)), fold(one(along)))

    arrive_all(COT)
    arrive_all(HID2)

    def put_c(dst):
        def use(row, value, mid, keep):
            dst[pl.ds(row, R), :] = value.astype(BF16)

        return use

    each_halo(COT, put_c(vh_c), put_c(vo_c))

    def put_s(n_dst, s_dst, c_src):
        def use(row, value, mid, keep):
            rows = pl.ds(row, R)
            normed = (value + (mid - center)) * inv2
            n_dst[rows, :] = normed
            s_dst[rows, :] = c_src[rows, :].astype(F32) * activate_slope(normed * gain2 + bias2)

        return use

    each_halo(HID2, put_s(n2h, s2h, vh_c), put_s(n2o, s2o, vo_c))
    leave(outb, o_ref)
    sums2 = stats_wait(2)

    def gradient(slope, normed, sums, factor):
        return factor * (slope - sums[0:1] / total - normed * (sums[1:2] / total))

    factor2 = gain2 * inv2

    def grad_rows(row, keep_own, keep_halo):
        rows = pl.ds(row, R)
        g = gradient(s2o[rows, :], n2o[rows, :], sums2, factor2)
        vo_g[rows, :] = (g if keep_own is None else jnp.where(keep_own, g, 0.0)).astype(BF16)
        g = gradient(s2h[rows, :], n2h[rows, :], sums2, factor2)
        vh_g[rows, :] = jnp.where(keep_halo, g, 0.0).astype(BF16)

    def grad_two(c, carry):
        for k in range(CH):
            grad_rows(row_of(c * CH + k + 1), None, keep_h)
        return carry

    lax.fori_loop(0, NCH, grad_two, 0)
    for side in range(2):
        grad_rows(END[side] * R, keep_o[side], keep_ho[side])

    def back_step(c, slot, carry):
        plain, along = carry
        slopes = []
        for k, back in enumerate(conv_rows(vo_g, vh_g, wb2, c, slot)):
            rows = pl.ds(row_of(c * CH + k + 1), R)
            normed = n1o[rows, :]
            slope = back * activate_slope(normed * gain1 + bias1)
            s1o[rows, :] = slope
            plain = plain + eight(slope)
            along = along + eight(slope * normed)
            slopes.append(slope)
        return (plain, along), slopes

    plain, along = paired(SLO1, back_step, (zero8, zero8))
    stats_send(3, fold(one(plain)), fold(one(along)))
    forward(SLO1, ODD[: NCH // 4])
    kernel_terms(1, vt_a, vo_g, vh_g)
    forward(SLO1, ODD[NCH // 4 :])
    sums1 = stats_wait(3)
    arrive_all(SLO1)
    pieces_sum(1)
    factor1 = gain1 * inv1

    def put_g(dst, normed_ref):
        def use(row, value, mid, keep):
            rows = pl.ds(row, R)
            g = gradient(value + mid, normed_ref[rows, :], sums1, factor1)
            dst[rows, :] = jnp.where(keep, g, 0.0).astype(BF16)

        return use

    def grad_one(c, carry):
        for k in range(CH):
            rows = pl.ds(row_of(c * CH + k + 1), R)
            vo_g[rows, :] = gradient(s1o[rows, :], n1o[rows, :], sums1, factor1).astype(BF16)
        return carry

    lax.fori_loop(0, NCH, grad_one, 0)
    each_halo(SLO1, put_g(vh_g, n1h), put_g(vo_g, n1o))
    kernel_terms(0, vt_f, vo_g, vh_g)

    def last_loop(i, carry):
        for j in range(PAIR):
            c = i * PAIR + j
            for k, back in enumerate(conv_rows(vo_g, vh_g, wb1, c, j * CH)):
                outb[pl.ds(row_of(c * CH + k), R), :] = back.astype(BF16)
        return carry

    lax.fori_loop(0, NCH // PAIR, last_loop, 0)
    pieces_sum(0)
    leave(outb, fg_ref)
    for row, (sums, part) in enumerate(((sums1, 1), (sums1, 0), (sums2, 1), (sums2, 0))):
        ng_ref[row : row + 1, :] = sums[part : part + 1]
    pieces_out(1)
    pieces_out(0)
    for e in range(NEXCH):
        sent_all(e)
        forwarded(e)


def finish(scale, o_ref, fg_ref, dk_ref, ng_ref, oo_ref, ofg_ref, dk1_ref, dk2_ref, ong_ref, sem):
    C = o_ref.shape[0]
    copies = [
        pltpu.make_async_copy(o_ref, oo_ref, sem.at[0]),
        pltpu.make_async_copy(fg_ref, ofg_ref, sem.at[1]),
    ]
    for copy in copies:
        copy.start()
    for w, out_ref in enumerate((dk1_ref, dk2_ref)):
        for group in range(7):
            tall = jnp.transpose(dk_ref[w, group * C : (group + 1) * C].astype(F32)) * scale
            for slot in range(min(4, 27 - 4 * group)):
                out_ref[4 * group + slot] = tall[slot * C : (slot + 1) * C]
    ong_ref[...] = ng_ref[0:4, 0:C] * scale
    for copy in copies:
        copy.wait()


def local(features, kernel_one, gain_one, bias_one, kernel_two, gain_two, bias_two, cotangent):
    C, X, Y, Z = features.shape
    nx, ny = lax.axis_size("gx"), lax.axis_size("gy")
    n = nx * ny
    total = float(X * Y * Z * nx * ny)
    R = Z // 2
    NCH = Y // CH
    piece = -(-224 // (8 * n)) * 8
    taps = lambda k: jnp.transpose(k, (2, 3, 4, 0, 1)).reshape(27, C, C)
    row = lambda v: v.reshape(1, C)
    rows, all_rows = Y * R, (Y + 2) * R
    packed = CH * R // 2 + 16
    V = pltpu.VMEM
    DMA = pltpu.SemaphoreType.DMA
    scratch = [
        V((rows, L), F32), V((8, L), F32), V((R, 2 * Z), BF16), V((2 * L, 2 * Z), BF16),
        V((L, L), BF16), V((27, C, L), F32),
    ]
    scratch += [V((3, 2 * L, 2 * L), BF16)] * 4
    scratch += [V((all_rows, L), BF16)] * 8
    scratch += [V((2 * L, rows), BF16)] * 2
    scratch += [V((rows, L), F32)] * 2
    scratch += [V((all_rows, L), F32)] * 7
    scratch += [
        V((rows, L), BF16), V((2 * CH, R + 16, L), F32), V((NCH, L), F32), V((NCH, L), F32),
        V((NCH, L), F32), V((3, 2 * L, 2 * L), F32),
    ]
    scratch += [V((NEXCH, NCH, packed, L), BF16)] * 2 + [V((NEXCH, 3, R + 16, L), BF16)]
    scratch += [V((NEXCH, NCH, packed, L), BF16)] * 2 + [V((NEXCH, 2, R + 16, L), BF16)] * 3
    scratch += [DMA((NEXCH, 2 * NCH + 6))] * 2
    scratch += [V((4, 2, L), F32), V((4, n, 2, L), F32), DMA((4,)), DMA((4,))]
    scratch += [
        V((2, n, piece, L), F32), V((2, n, piece, L), F32), V((2, piece, L), BF16),
        V((2, n, piece, L), BF16), DMA((2, 2)), DMA((2, 2)),
        V((C, X, Y, Z), BF16), V((C, X, Y, Z), BF16), V((27, C, C), BF16), V((27, C, C), BF16),
        *[V((1, C), F32)] * 4, DMA((8,)), V((NEXCH, NCH // 2, packed, L), BF16),
        DMA((NEXCH, NCH // 2)), DMA((NEXCH, NCH // 2)),
    ]
    vmem = pl.BlockSpec(memory_space=pltpu.VMEM)
    anywhere = pl.BlockSpec(memory_space=pl.ANY)
    volume = jax.ShapeDtypeStruct((C, X, Y, Z), BF16)
    mids = pl.pallas_call(
        functools.partial(kernel, nx, ny, total),
        name="blocks",
        out_shape=[
            volume, volume, jax.ShapeDtypeStruct((2, n * piece, L), BF16),
            jax.ShapeDtypeStruct((8, L), F32),
        ],
        in_specs=[pl.BlockSpec(memory_space=pltpu.HBM)] * 8,
        out_specs=[vmem] * 4,
        scratch_shapes=scratch,
        compiler_params=pltpu.CompilerParams(
            collective_id=0, has_side_effects=True, vmem_limit_bytes=48 << 20
        ),
    )(
        *[
            pltpu.with_memory_space_constraint(v, pltpu.HBM)
            for v in (
                features, cotangent, taps(kernel_one), taps(kernel_two),
                row(gain_one), row(bias_one), row(gain_two), row(bias_two),
            )
        ]
    )
    terms = jax.ShapeDtypeStruct((27, C, C), F32)
    out, fg, dk1, dk2, norm = pl.pallas_call(
        functools.partial(finish, total ** -0.5),
        name="finish",
        out_shape=[volume, volume, terms, terms, jax.ShapeDtypeStruct((4, C), F32)],
        in_specs=[anywhere] * 2 + [vmem] * 2,
        out_specs=[anywhere] * 2 + [vmem] * 3,
        scratch_shapes=[DMA((2,))],
        compiler_params=pltpu.CompilerParams(vmem_limit_bytes=8 << 20),
    )(*mids)
    untap = lambda d: jnp.transpose(d.reshape(3, 3, 3, C, C), (3, 4, 0, 1, 2))
    return out, fg, untap(dk1), untap(dk2), norm


def solution(mesh):
    in_specs = (P(None, "gx", "gy", None), P(), P(), P(), P(), P(), P(), P(None, "gx", "gy", None))
    out_specs = (P(None, "gx", "gy", None), P(None, "gx", "gy", None), P(), P(), P())
    return jax.shard_map(local, mesh=mesh, in_specs=in_specs, out_specs=out_specs, check_vma=False)
```

```python
import functools

import jax
import jax.numpy as jnp
from jax import lax
from jax.experimental import pallas as pl
from jax.experimental.pallas import tpu as pltpu
from jax.sharding import PartitionSpec as P

EPSILON = 1e-05
SLOPE = 0.01
SHARPNESS = 8.0
MESH = pl.DeviceIdType.MESH
LOGICAL = pl.DeviceIdType.LOGICAL
F32 = jnp.float32
BF16 = jnp.bfloat16
L = 128
CH = 4
FEAT, COT, HID1, HID2, SLO1 = range(5)
NEXCH = 5
NT = (((1,), (1,)), ((), ()))


def activate(s):
    scaled = SHARPNESS * s
    soft = jnp.maximum(scaled, 0.0) + jnp.log(1.0 + jnp.exp(-jnp.abs(scaled)))
    return SLOPE * s + ((1.0 - SLOPE) / SHARPNESS) * soft


def activate_slope(s):
    half = 0.5 * (1.0 - SLOPE)
    return (SLOPE + half) + half * jnp.tanh((0.5 * SHARPNESS) * s)


def untap(flat, out_ref, scale):
    C = out_ref.shape[1]
    for group in range(7):
        tall = jnp.transpose(flat[group * C : (group + 1) * C].astype(F32)) * scale
        for slot in range(min(4, 27 - 4 * group)):
            out_ref[4 * group + slot] = tall[slot * C : (slot + 1) * C]


def kernel(
    nx, ny, total,
    f_hbm, c_hbm, k1_hbm, k2_hbm, g1_hbm, b1_hbm, g2_hbm, b2_hbm,
    o_ref, fg_ref, dk1_ref, dk2_ref, ng_ref,
    t1, par, e_mat, s_mat, i_mat, base, wf1, wf2, wb2, wb1,
    vo_f, vh_f, vo_c, vh_c, vo_a, vh_a, vo_g, vh_g, vt_f, vt_a,
    hc1, hc2, n1o, n1h, n2o, n2h, s2o, s2h, s1o, outb, bs, mcs, scs, mcs1, raw,
    spr, spl, se, rl, rr, re, rdl, rdr, hs_sem, hr_sem,
    msg, st, ss_sem, sr_sem,
    pk, rsb, ags, agb, ws_sem, wr_sem,
    f_ref, c_ref, k1_ref, k2_ref, g1_ref, b1_ref, g2_ref, b2_ref, in_sem, rel, rel_sem, fwd_sem,
):
    C, X, Y, Z = f_ref.shape
    R = Z // 2
    CR = CH * R
    NCH = Y // CH
    n = nx * ny
    PIECE = rsb.shape[2]
    gx, gy = lax.axis_index("gx"), lax.axis_index("gy")
    me = gx * ny + gy
    has_l, has_r = gx > 0, gx < nx - 1
    has_d, has_u = gy > 0, gy < ny - 1

    def peer(k):
        other = me + k
        return jnp.where(other >= n, other - n, other)

    def others(use):
        if n & (n - 1):
            lax.fori_loop(1, n, lambda k, carry: (use(peer(k)), carry)[1], 0)
            return
        for dy in range(ny - 1, -1, -1):
            def body(t, carry, dy=dy):
                use(jnp.bitwise_xor(me, (nx - 1 - t) * ny + dy))
                return carry

            lax.fori_loop(0, nx if dy else nx - 1, body, 0)

    fetch = [
        pltpu.make_async_copy(src, dst, in_sem.at[k])
        for k, (src, dst) in enumerate(
            (
                (f_hbm, f_ref), (k1_hbm, k1_ref), (k2_hbm, k2_ref), (c_hbm, c_ref),
                (g1_hbm, g1_ref), (b1_hbm, b1_ref), (g2_hbm, g2_ref), (b2_hbm, b2_ref),
            )
        )
    ]
    for copy in fetch:
        copy.start()

    barrier = pltpu.get_barrier_semaphore()

    others(
        lambda d: pl.semaphore_signal(barrier, inc=1, device_id=d, device_id_type=LOGICAL)
    )

    lane = lax.broadcasted_iota(jnp.int32, (1, L), 1)
    xb = lax.rem(lane // C, 2) == 1
    z0 = lane < L // 2
    flag = lambda b: jnp.where(b, 1, 0)
    keep_h = jnp.where(xb, flag(has_l), flag(has_r)) > 0
    full_y = jnp.full((1, L), 1, jnp.int32)
    keep_o = [full_y * flag(has_d) > 0, full_y * flag(has_u) > 0]
    keep_ho = [(jnp.where(xb, flag(has_l), flag(has_r)) * flag(b)) > 0 for b in (has_d, has_u)]

    def row_of(y):
        return pl.multiple_of(y * R, R)

    def fold(v):
        v = v + pltpu.roll(v, C, 1)
        return v + pltpu.roll(v, 2 * C, 1)

    def loop(count, body, carry=0, unroll=1):
        def group(i, carry):
            for k in range(unroll):
                carry = body(i * unroll + k, carry)
            return carry

        return lax.fori_loop(0, count // unroll, group, carry)

    def eight(v):
        return jnp.sum(v.reshape(v.shape[0] // 8, 8, L), axis=0)

    def one(v):
        return jnp.sum(v, axis=0, keepdims=True)

    r_i = lax.broadcasted_iota(jnp.int32, (R, 2 * Z), 0)
    c_i = lax.broadcasted_iota(jnp.int32, (R, 2 * Z), 1)
    e_mat[...] = jnp.where(
        lax.rem(c_i, Z) == 2 * r_i + c_i // Z, 1.0, 0.0
    ).astype(BF16)
    r_i = lax.broadcasted_iota(jnp.int32, (2 * L, 2 * Z), 0)
    c_i = lax.broadcasted_iota(jnp.int32, (2 * L, 2 * Z), 1)
    same = lax.rem(r_i // R, 2) == c_i // Z
    s_mat[...] = jnp.where(
        same & (lax.rem(c_i, Z) == 2 * lax.rem(r_i, R) + r_i // L), 1.0, 0.0
    ).astype(BF16)
    r_i = lax.broadcasted_iota(jnp.int32, (L, L), 0)
    c_i = lax.broadcasted_iota(jnp.int32, (L, L), 1)
    i_mat[...] = jnp.where(r_i == c_i, 1.0, 0.0).astype(BF16)
    bs[...] = jnp.zeros(bs.shape, F32)

    spots_in = [(0, 0, z, x) for z in range(2) for x in range(2)]
    halo_x = {0: 2, 1: -1}
    rows_in = [(x, z) for _, _, z, x in spots_in] + [(halo_x[x], z) for _, _, z, x in spots_in]
    cols_a = [(x, z) for _, _, z, x in spots_in]
    cols_b = [(x, 2 if z == 0 else -1) for _, _, z, x in spots_in]

    def build(k_ref, w_ref, forward):
        if forward:
            stacked = jnp.concatenate([k_ref[t] for t in range(27) for _ in range(4)], axis=0)
            wide = lax.dot_general(
                i_mat[0:C, 0:C], stacked, NT, preferred_element_type=F32
            )
            for t in range(27):
                base[t] = wide[:, t * L : (t + 1) * L]
        else:
            r4 = lax.broadcasted_iota(jnp.int32, (C, L), 0)
            c4 = lax.rem(lax.broadcasted_iota(jnp.int32, (C, L), 1), C)
            spread4 = jnp.where(r4 == c4, 1.0, 0.0).astype(BF16)
            tall = k_ref[...].reshape(27 * C, C)
            wide = jnp.dot(tall, spread4, preferred_element_type=F32)
            for t in range(27):
                base[t] = wide[t * C : (t + 1) * C]
        block = lax.broadcasted_iota(jnp.int32, (C, L), 1) // C

        def one_row(j, carry):
            dy = j if forward else 2 - j
            for kb, (xi, zi) in enumerate(rows_in):
                for t, cols in enumerate((cols_a, cols_b)):
                    value = jnp.zeros((C, L), F32)
                    for b, (xo, zo) in enumerate(cols):
                        dx, dz = xi - xo + 1, zi - zo + 1
                        if not forward:
                            dx, dz = 2 - dx, 2 - dz
                        if 0 <= dx <= 2 and 0 <= dz <= 2:
                            tap = base[dx * 9 + dy * 3 + dz]
                            value = jnp.where(block == b, tap, value)
                    w_ref[j, kb * C : (kb + 1) * C, t * L : (t + 1) * L] = value.astype(BF16)
            return carry

        lax.fori_loop(0, 3, one_row, 0)

    def enter(in_ref, vo, e, after=None):
        def widen(c, carry):
            t1[pl.ds(pl.multiple_of(c * X * Y, X * Y), X * Y), :] = (
                in_ref[c].reshape(X * Y, Z).astype(F32)
            )
            return carry

        loop(C, widen, unroll=4)
        zero = jnp.zeros((X * C, Z), BF16)

        def chunk(c, carry):
            vs = []
            for k in range(CH):
                y = c * CH + k
                x0 = t1[pl.ds(y, C, stride=X * Y), :]
                x1 = t1[pl.ds(Y + y, C, stride=X * Y), :]
                xy = jnp.concatenate([x0, x1], axis=0).astype(BF16)
                rhs = jnp.concatenate(
                    [jnp.concatenate([xy, zero], axis=1), jnp.concatenate([zero, xy], axis=1)],
                    axis=0,
                )
                v = lax.dot_general(e_mat[...], rhs, NT, preferred_element_type=F32)
                vo[pl.ds(row_of(y + 1), R), :] = v.astype(BF16)
                vs.append(v)
            pack(e, c, vs, None)
            return carry

        for part in range(2):
            lax.fori_loop(
                part * NCH // 4, (part + 1) * NCH // 4,
                lambda h, carry: chunk(2 * h + 1, chunk(2 * h, carry)), 0,
            )
            if after is not None:
                after(part)

    def leave(src, dst):
        def pair(p, carry):
            o = src[pl.ds(pl.multiple_of(p * L, L), L), :]
            d = lax.dot_general(i_mat[...], o, NT, preferred_element_type=F32).astype(BF16)
            both = jnp.concatenate([d[: L // 2], d[L // 2 :]], axis=1)
            xs = jnp.dot(both, s_mat[...], preferred_element_type=F32)
            r0 = pl.multiple_of(p * 2 * R, 2 * R)
            t1[pl.ds(r0, R), :] = xs[:, :Z]
            t1[pl.ds(r0 + R, R), :] = xs[:, Z:]
            return carry

        with jax.named_scope("leave_pairs"):
            loop(Y // 2, pair, unroll=4)

        def channel(c, carry):
            for x in range(X):
                dst[c, x] = t1[pl.ds(x * C + c, Y, stride=X * C), :].astype(BF16)
            return carry

        with jax.named_scope("leave_channels"):
            loop(C, channel, unroll=4)

    def flip(vo, vt):
        def pair(p, carry):
            rows = vo[pl.ds(row_of(2 * p + 1), 2 * R), :]
            wide = rows.astype(F32)
            slot = 2 * lax.rem(p, 4)
            for k in range(2):
                bs[slot + k, 8 : 8 + R, :] = wide[k * R : (k + 1) * R]
            shifted = jnp.concatenate(
                [jnp.where(z0, bs[slot + k, 9 : 9 + R, :], bs[slot + k, 7 : 7 + R, :]) for k in range(2)],
                axis=0,
            ).astype(BF16)
            cols = pl.ds(pl.multiple_of(p * 2 * R, 2 * R), 2 * R)
            for k, part in enumerate((rows, shifted)):
                vt[k * L : (k + 1) * L, cols] = lax.dot_general(
                    i_mat[...], part, NT, preferred_element_type=F32
                ).astype(BF16)
            return carry

        loop(Y // 2, pair, unroll=4)

    half = CR // 2

    def pack(e, c, vs, center):
        for p in range(CH // 2):
            a, b = vs[2 * p], vs[2 * p + 1]
            rows = slice(p * (R + 16), p * (R + 16) + R)
            spr[e, c, rows, :] = jnp.where(xb, a, pltpu.roll(b, L - C, 1)).astype(BF16)
            spl[e, c, rows, :] = jnp.where(xb, pltpu.roll(b, C, 1), a).astype(BF16)
        if center is not None:
            center = center.astype(BF16)
            spr[e, c, R : R + 16, :] = center
            spl[e, c, R : R + 16, :] = center

        first = 2 if isinstance(c, int) and c else jnp.where(c == 0, 0, 2)
        se[e, first, 0:R, :] = vs[0].astype(BF16)
        if center is not None:
            se[e, first, R : R + 16, :] = center
        last = jnp.where(c == NCH - 1, 1, 2)
        se[e, last, 0:R, :] = vs[CH - 1].astype(BF16)
        if center is not None:
            se[e, last, R : R + 16, :] = center

    def copy_of(e, index, src, dst, dx, dy):
        return lambda: pltpu.make_async_remote_copy(
            src_ref=src, dst_ref=dst,
            send_sem=hs_sem.at[e, index], recv_sem=hr_sem.at[e, index],
            device_id=(lax.rem(gx + dx + nx, nx), lax.rem(gy + dy + ny, ny)),
            device_id_type=MESH,
        )

    def side_copies(e, c):
        return [
            (has_r, has_l, copy_of(e, c, spr.at[e, c], rl.at[e, c], 1, 0)),
            (has_l, has_r, copy_of(e, NCH + c, spl.at[e, c], rr.at[e, c], -1, 0)),
        ]

    def end_copies(e):
        low, high = pl.ds(0, R + 16), pl.ds(R, R + 16)
        both = jnp.logical_and
        m = 2 * NCH
        last = NCH - 1
        return [
            [
                (has_d, has_u, copy_of(e, m, se.at[e, 0], re.at[e, 1], 0, -1)),
                (both(has_r, has_d), both(has_l, has_u),
                 copy_of(e, m + 2, spr.at[e, 0, low], rdl.at[e, 1], 1, -1)),
                (both(has_l, has_d), both(has_r, has_u),
                 copy_of(e, m + 4, spl.at[e, 0, low], rdr.at[e, 1], -1, -1)),
            ],
            [
                (has_u, has_d, copy_of(e, m + 1, se.at[e, 1], re.at[e, 0], 0, 1)),
                (both(has_r, has_u), both(has_l, has_d),
                 copy_of(e, m + 3, spr.at[e, last, high], rdl.at[e, 0], 1, 1)),
                (both(has_l, has_u), both(has_r, has_d),
                 copy_of(e, m + 5, spl.at[e, last, high], rdr.at[e, 0], -1, 1)),
            ],
        ]

    def start(copies):
        for sends, _, copy in copies:
            @pl.when(sends)
            def _(copy=copy):
                copy().start()

    def arrive(copies):
        for _, takes, copy in copies:
            @pl.when(takes)
            def _(copy=copy):
                copy().wait_recv()

    RELAY = nx == 8
    ODD = range(NCH // 2)
    low_mid, high_mid = nx // 2 - 1, nx // 2

    def hop(e, h, src, dst, there, s_sem, r_sem):
        return pltpu.make_async_remote_copy(
            src_ref=src, dst_ref=dst, send_sem=s_sem, recv_sem=r_sem,
            device_id=(there, gy), device_id_type=MESH,
        )

    def send_odd(e, c):
        h = c // 2
        (_, _, right), (_, _, left) = side_copies(e, c)
        relays = (
            (gx == low_mid, has_r, right, spr, nx - 1, hs_sem.at[e, c]),
            (gx == high_mid, has_l, left, spl, 0, hs_sem.at[e, NCH + c]),
        )
        for via, sends, direct, src, there, s_sem in relays:
            @pl.when(via)
            def _(src=src, there=there, s_sem=s_sem):
                hop(e, h, src.at[e, c], rel.at[e, h], there, s_sem, rel_sem.at[e, h]).start()

            @pl.when(jnp.logical_and(sends, jnp.logical_not(via)))
            def _(direct=direct):
                direct().start()

    def forwards(e, h):
        c = 2 * h + 1
        return (
            (gx == nx - 1, hop(e, h, rel.at[e, h], rl.at[e, c], high_mid, fwd_sem.at[e, h], hr_sem.at[e, c])),
            (gx == 0, hop(e, h, rel.at[e, h], rr.at[e, c], low_mid, fwd_sem.at[e, h], hr_sem.at[e, NCH + c])),
        ) if RELAY else ()

    def relay_arrives(e, h):
        hop(e, h, rel.at[e, h], rel.at[e, h], low_mid, fwd_sem.at[e, h], rel_sem.at[e, h]).wait_recv()

    def forward(e, which):
        for h in which:
            for here, copy in forwards(e, h):
                @pl.when(here)
                def _(h=h, copy=copy):
                    relay_arrives(e, h)
                    copy.start()

    def forwarded(e):
        for h in ODD:
            for here, copy in forwards(e, h):
                @pl.when(here)
                def _(copy=copy):
                    copy.wait_send()

    def send(e, c, odd):
        if RELAY and odd:
            send_odd(e, c)
        else:
            start(side_copies(e, c))

    def send_ends(e):
        for copies in end_copies(e):
            start(copies)

    def send_part(e, low, high):
        def body(h, carry):
            send(e, 2 * h, False)
            send(e, 2 * h + 1, True)
            return carry

        lax.fori_loop(low, high, body, 0)

    def send_all(e):
        send_part(e, 0, NCH // 2)
        send_ends(e)

    def arrive_ends(e):
        for copies in end_copies(e):
            arrive(copies)

    def arrive_all(e):
        def body(c, carry):
            arrive(side_copies(e, c))
            return carry

        lax.fori_loop(0, NCH, body, 0)
        arrive_ends(e)

    def sent_all(e):
        def done(copies):
            for sends, _, copy in copies:
                @pl.when(sends)
                def _(copy=copy):
                    copy().wait_send()

        def body(c, carry):
            done(side_copies(e, c))
            return carry

        lax.fori_loop(0, NCH, body, 0)
        for copies in end_copies(e):
            done(copies)

    def center_of(tile):
        wide = tile.astype(F32)
        return (wide[0:8] + wide[8:16])[0:1]

    def halo_rows(e, c):
        center = jnp.where(xb, center_of(rl[e, c, R : R + 16, :]), center_of(rr[e, c, R : R + 16, :]))
        found = []
        for p in range(CH // 2):
            rows = slice(p * (R + 16), p * (R + 16) + R)
            a, b = rl[e, c, rows, :].astype(F32), rr[e, c, rows, :].astype(F32)
            found.append(jnp.where(xb, a, b))
            found.append(jnp.where(xb, pltpu.roll(a, C, 1), pltpu.roll(b, L - C, 1)))
        return found, center

    def end_rows(e, side):
        own, own_center = re[e, side, 0:R, :].astype(F32), center_of(re[e, side, R : R + 16, :])
        data, tile = (slice(16, 16 + R), slice(0, 16)) if side == 0 else (slice(0, R), slice(R, R + 16))
        a, b = rdl[e, side, data, :].astype(F32), rdr[e, side, data, :].astype(F32)
        center = jnp.where(xb, center_of(rdl[e, side, tile, :]), center_of(rdr[e, side, tile, :]))
        if side == 0:
            a, b = pltpu.roll(a, C, 1), pltpu.roll(b, L - C, 1)
        return own, own_center, jnp.where(xb, a, b), center

    END = (0, Y + 1)

    def each_halo(e, use_halo, use_own):
        def body(c, carry):
            found, center = halo_rows(e, c)
            for k, value in enumerate(found):
                use_halo(row_of(c * CH + k + 1), value, center, keep_h)
            return carry

        lax.fori_loop(0, NCH, body, 0)
        each_end(e, use_halo, use_own)

    def each_end(e, use_halo, use_own):
        for side in range(2):
            own, own_center, value, center = end_rows(e, side)
            use_own(END[side] * R, own, own_center, keep_o[side])
            use_halo(END[side] * R, value, center, keep_ho[side])

    def stats_send(r, top, low):
        row = lax.broadcasted_iota(jnp.int32, (2, L), 0)
        both = jnp.where(row == 0, top, low)
        msg[r] = both
        st[r, me] = both

        others(
            lambda d: pltpu.make_async_remote_copy(
                src_ref=msg.at[r], dst_ref=st.at[r, me],
                send_sem=ss_sem.at[r], recv_sem=sr_sem.at[r],
                device_id=d, device_id_type=LOGICAL,
            ).start()
        )

    def stats_wait(r):
        rest = st.at[r, pl.ds(0, n - 1)]
        pltpu.make_async_remote_copy(
            src_ref=rest, dst_ref=rest, send_sem=ss_sem.at[r], recv_sem=sr_sem.at[r],
            device_id=peer(1), device_id_type=LOGICAL,
        ).wait()
        return jnp.sum(st[r], axis=0)

    def pieces_send(w, phase):
        others(
            lambda d: pltpu.make_async_remote_copy(
                src_ref=pk.at[w, d] if phase == 0 else ags.at[w],
                dst_ref=(rsb if phase == 0 else agb).at[w, me],
                send_sem=ws_sem.at[w, phase], recv_sem=wr_sem.at[w, phase],
                device_id=d, device_id_type=LOGICAL,
            ).start()
        )

    def pieces_wait(w, phase):
        rest = (rsb if phase == 0 else agb).at[w, pl.ds(0, n - 1)]
        pltpu.make_async_remote_copy(
            src_ref=rest, dst_ref=rest,
            send_sem=ws_sem.at[w, phase], recv_sem=wr_sem.at[w, phase],
            device_id=peer(1), device_id_type=LOGICAL,
        ).wait()

    def kernel_products(vt, vo, vh):
        for j in range(3):
            g = jnp.concatenate([vo[j * R : (j + Y) * R, :], vh[j * R : (j + Y) * R, :]], axis=1)
            raw[j] = jnp.dot(vt[...], g, preferred_element_type=F32)

    def kernel_terms(w):
        block = lax.broadcasted_iota(jnp.int32, (C, L), 1) // C
        rows_v = cols_a + cols_b
        groups = [jnp.zeros((C, L), F32) for _ in range(7)]
        for j in range(3):
            dy = 2 - j
            for dx in range(3):
                for dz in range(3):
                    tap = dx * 9 + dy * 3 + dz
                    group, slot = tap // 4, tap % 4
                    for kb, (xv, zv) in enumerate(rows_v):
                        for cb, (xg, zg) in enumerate(rows_in):
                            if kb >= 4 and zv == 2 and zg != 1:
                                continue
                            if kb >= 4 and zv == -1 and zg != 0:
                                continue
                            if xv - xg + 1 != dx or zv - zg + 1 != dz:
                                continue
                            t, b = cb // 4, cb % 4
                            part = raw[j, kb * C : (kb + 1) * C, t * L : (t + 1) * L]
                            if slot != b:
                                part = pltpu.roll(part, (slot - b) % 4 * C, 1)
                            groups[group] = groups[group] + jnp.where(block == slot, part, 0.0)
        flat = jnp.concatenate(groups, axis=0)
        rows = n * PIECE
        if rows > flat.shape[0]:
            flat = jnp.concatenate([flat, jnp.zeros((rows - flat.shape[0], L), F32)], axis=0)
        pk[w] = flat.reshape(n, PIECE, L)
        rsb[w, me] = pk[w, me]

    def pieces_sum(w):
        pieces_wait(w, 0)
        whole = jnp.sum(rsb[w], axis=0).astype(BF16)
        ags[w] = whole
        agb[w, me] = whole
        pieces_send(w, 1)

    dk_refs = (dk1_ref, dk2_ref)

    def pieces_out(w):
        pieces_wait(w, 1)
        untap(agb[w].reshape(n * PIECE, L), dk_refs[w], total ** -0.5)

    def conv_rows(vo, vh, w_ref, c, slot=0):
        parts = []
        for j in range(3):
            rows = pl.ds(row_of(c * CH + j), CR)
            parts += [vo[rows, :], vh[rows, :]]
        ab = jnp.dot(
            jnp.concatenate(parts, axis=1), w_ref[...].reshape(6 * L, 2 * L),
            preferred_element_type=F32,
        )
        for k in range(CH):
            bs[slot + k, 8 : 8 + R, :] = ab[k * R : (k + 1) * R, L:]
        return [
            ab[k * R : (k + 1) * R, :L]
            + jnp.where(z0, bs[slot + k, 7 : 7 + R, :], bs[slot + k, 9 : 9 + R, :])
            for k in range(CH)
        ]

    def totals(vs):
        return fold(one(functools.reduce(jnp.add, [eight(v) for v in vs])))

    def center_near(s):
        mean = s / (4.0 * CR)
        high = mean.astype(BF16).astype(F32)
        low = (mean - high).astype(BF16).astype(F32)
        tile = jnp.concatenate(
            [jnp.broadcast_to(high, (8, L)), jnp.broadcast_to(low, (8, L))], axis=0
        )
        return high + low, tile

    cells = float(X * Y * Z)
    zero8 = jnp.zeros((8, L), F32)
    PAIR = 2

    def paired(e, step, carry, before=None, after=None):
        def group(i, carry, first):
            inner, s = carry
            if before is not None:
                before(i)
            found = []
            for k in range(PAIR):
                inner, vs = step(i * PAIR + k, k * CH, inner)
                found.append((vs, totals(vs)))
            if after is not None:
                after(i)
            center, tile = center_near(found[0][1] if first else s)
            for k, (vs, s) in enumerate(found):
                c = i * PAIR + k
                centers_of[e][pl.ds(c, 1), :] = center
                scs[pl.ds(c, 1), :] = s
                inner = keep_chunk(e, c, vs, center, tile, inner)
            if e != HID2 and i < EARLY:
                for k in range(PAIR):
                    send(e, i * PAIR + k, k % 2 == 1)
            return inner, s

        carry = group(0, (carry, None), True)
        for i in range(1, NCH // PAIR):
            carry = group(i, carry, False)
        return carry[0]

    EARLY = NCH // PAIR // 2

    def send_late(e):
        for i in range(EARLY, NCH // PAIR):
            for k in range(PAIR):
                send(e, i * PAIR + k, k % 2 == 1)
        send_ends(e)

    centers_of = {HID1: mcs1, HID2: mcs, SLO1: mcs}

    def keep_chunk(e, c, vs, center, tile, inner):
        vs = [v - center for v in vs]
        pack(e, c, vs, tile)
        if e != SLO1:
            hc = hc1 if e == HID1 else hc2
            for k, v in enumerate(vs):
                hc[pl.ds(row_of(c * CH + k), R), :] = v
                inner = inner + eight(v * v)
        return inner

    def forward_loop(vo, vh, w_ref, e, before=None, after=None):
        def step(c, slot, squares):
            return squares, conv_rows(vo, vh, w_ref, c, slot)

        squares = fold(one(paired(e, step, zero8, before, after)))
        centers = centers_of[e][...]
        mean = one(scs[...]) / cells
        off = centers - mean
        rest = scs[...] - (4.0 * CR) * centers
        spread = squares + one(off * (2.0 * rest + (4.0 * CR) * off))
        return mean, spread

    def moments(r):
        sums = stats_wait(r)
        center = sums[0:1] / n

        def body(d, acc):
            off = st[r, d] - center
            return acc + off * off

        between = lax.fori_loop(0, n, body, jnp.zeros((2, L), F32))[0:1]
        variance = (sums[1:2] + cells * between) / total
        return center, lax.rsqrt(variance + EPSILON)

    fetch[0].wait()

    def send_f(part):
        if part == 0:
            pl.semaphore_wait(barrier, n - 1)
        send_part(FEAT, part * NCH // 4, (part + 1) * NCH // 4)

    enter(f_ref, vo_f, FEAT, send_f)
    send_ends(FEAT)
    fetch[1].wait()
    build(k1_ref, wf1, True)
    fetch[2].wait()
    build(k2_ref, wf2, True)
    build(k2_ref, wb2, False)
    build(k1_ref, wb1, False)
    fetch[3].wait()
    forward(FEAT, ODD[: NCH // 4])
    enter(c_ref, vo_c, COT)
    forward(FEAT, ODD[NCH // 4 :])

    def put_f(dst):
        def use(row, value, center, keep):
            dst[pl.ds(row, R), :] = jnp.where(keep, value, 0.0).astype(BF16)

        return use

    arrive_ends(FEAT)
    each_end(FEAT, put_f(vh_f), put_f(vo_f))

    def take_f(c):
        found, _ = halo_rows(FEAT, c)
        for k, value in enumerate(found):
            put_f(vh_f)(row_of(c * CH + k + 1), value, None, keep_h)

    arrive(side_copies(FEAT, 0))
    take_f(0)

    def before_f(i):
        for c in range(i * PAIR + 1, min(i * PAIR + PAIR + 1, NCH)):
            arrive(side_copies(FEAT, c))
            take_f(c)

    mean, spread = forward_loop(vo_f, vh_f, wf1, HID1, before_f)
    stats_send(0, mean, spread)
    send_late(HID1)
    for copy in fetch[4:]:
        copy.wait()
    par[...] = jnp.zeros(par.shape, F32)
    for row, ref in enumerate((g1_ref, b1_ref, g2_ref, b2_ref)):
        par[row : row + 1, 0:C] = ref[...]
    params = fold(par[...])
    gain1, bias1, gain2, bias2 = [params[r : r + 1] for r in range(4)]
    flip(vo_f, vt_f)
    forward(HID1, ODD)
    send_all(COT)
    center, inv1 = moments(0)
    arrive_all(HID1)

    def put_a(n_dst, v_dst, inv, gain, bias, center):
        def use(row, value, mid, keep):
            normed = (value + (mid - center)) * inv
            n_dst[pl.ds(row, R), :] = normed
            a = activate(normed * gain + bias)
            v_dst[pl.ds(row, R), :] = (a if keep is None else jnp.where(keep, a, 0.0)).astype(BF16)

        return use

    own_a = put_a(n1o, vo_a, inv1, gain1, bias1, center)

    halo_a = put_a(n1h, vh_a, inv1, gain1, bias1, center)

    def active_chunk(c):
        mid = mcs1[c : c + 1, :]
        for k in range(CH):
            own_a(row_of(c * CH + k + 1), hc1[pl.ds(row_of(c * CH + k), R), :], mid, None)
        found, mid = halo_rows(HID1, c)
        for k, value in enumerate(found):
            halo_a(row_of(c * CH + k + 1), value, mid, keep_h)

    def after_a(i):
        for c in range(PAIR * (i + 1) + 1, min(PAIR * (i + 2) + 1, NCH)):
            active_chunk(c)

    each_end(HID1, halo_a, own_a)
    for c in range(min(PAIR + 1, NCH)):
        active_chunk(c)

    mean, spread = forward_loop(vo_a, vh_a, wf2, HID2, after=after_a)
    stats_send(1, mean, spread)
    send_all(HID2)
    flip(vo_a, vt_a)
    forward(COT, ODD)
    center, inv2 = moments(1)

    def own_output(c, carry):
        plain, along = carry
        mid = mcs[pl.ds(c, 1), :]
        for k in range(CH):
            y = c * CH + k
            normed = (hc2[pl.ds(row_of(y), R), :] + (mid - center)) * inv2
            shifted = normed * gain2 + bias2
            outb[pl.ds(row_of(y), R), :] = activate(shifted).astype(BF16)
            rows = pl.ds(row_of(y + 1), R)
            slope = vo_c[rows, :].astype(F32) * activate_slope(shifted)
            n2o[rows, :] = normed
            s2o[rows, :] = slope
            plain = plain + eight(slope)
            along = along + eight(slope * normed)
        return plain, along

    plain, along = lax.fori_loop(0, NCH, own_output, (zero8, zero8))
    stats_send(2, fold(one(plain)), fold(one(along)))

    forward(HID2, ODD)
    leave(outb, o_ref)
    arrive_all(COT)
    arrive_all(HID2)

    def put_c(dst):
        def use(row, value, mid, keep):
            dst[pl.ds(row, R), :] = value.astype(BF16)

        return use

    each_halo(COT, put_c(vh_c), put_c(vo_c))

    def put_s(n_dst, s_dst, c_src):
        def use(row, value, mid, keep):
            rows = pl.ds(row, R)
            normed = (value + (mid - center)) * inv2
            n_dst[rows, :] = normed
            s_dst[rows, :] = c_src[rows, :].astype(F32) * activate_slope(normed * gain2 + bias2)

        return use

    each_halo(HID2, put_s(n2h, s2h, vh_c), put_s(n2o, s2o, vo_c))
    sums2 = stats_wait(2)

    def gradient(slope, normed, sums, factor):
        return factor * (slope - sums[0:1] / total - normed * (sums[1:2] / total))

    factor2 = gain2 * inv2

    def grad_rows(row, keep_own, keep_halo):
        rows = pl.ds(row, R)
        g = gradient(s2o[rows, :], n2o[rows, :], sums2, factor2)
        vo_g[rows, :] = (g if keep_own is None else jnp.where(keep_own, g, 0.0)).astype(BF16)
        g = gradient(s2h[rows, :], n2h[rows, :], sums2, factor2)
        vh_g[rows, :] = jnp.where(keep_halo, g, 0.0).astype(BF16)

    def grad_two(c, carry):
        for k in range(CH):
            grad_rows(row_of(c * CH + k + 1), None, keep_h)
        return carry

    lax.fori_loop(0, NCH, grad_two, 0)
    for side in range(2):
        grad_rows(END[side] * R, keep_o[side], keep_ho[side])

    def back_step(c, slot, carry):
        plain, along = carry
        slopes = []
        for k, back in enumerate(conv_rows(vo_g, vh_g, wb2, c, slot)):
            rows = pl.ds(row_of(c * CH + k + 1), R)
            normed = n1o[rows, :]
            slope = back * activate_slope(normed * gain1 + bias1)
            s1o[rows, :] = slope
            plain = plain + eight(slope)
            along = along + eight(slope * normed)
            slopes.append(slope)
        return (plain, along), slopes

    plain, along = paired(SLO1, back_step, (zero8, zero8))
    stats_send(3, fold(one(plain)), fold(one(along)))
    send_late(SLO1)
    kernel_products(vt_a, vo_g, vh_g)
    forward(SLO1, ODD[: NCH // 4])
    kernel_terms(1)
    forward(SLO1, ODD[NCH // 4 :])
    sums1 = stats_wait(3)
    arrive_all(SLO1)
    pieces_send(1, 0)
    factor1 = gain1 * inv1

    def put_g(dst, normed_ref):
        def use(row, value, mid, keep):
            rows = pl.ds(row, R)
            g = gradient(value + mid, normed_ref[rows, :], sums1, factor1)
            dst[rows, :] = jnp.where(keep, g, 0.0).astype(BF16)

        return use

    def grad_one(c, carry):
        for k in range(CH):
            rows = pl.ds(row_of(c * CH + k + 1), R)
            vo_g[rows, :] = gradient(s1o[rows, :], n1o[rows, :], sums1, factor1).astype(BF16)
        return carry

    lax.fori_loop(0, NCH, grad_one, 0)
    each_halo(SLO1, put_g(vh_g, n1h), put_g(vo_g, n1o))
    kernel_products(vt_f, vo_g, vh_g)
    kernel_terms(0)
    pieces_send(0, 0)

    def last_loop(i, carry):
        for j in range(PAIR):
            c = i * PAIR + j
            for k, back in enumerate(conv_rows(vo_g, vh_g, wb1, c, j * CH)):
                outb[pl.ds(row_of(c * CH + k), R), :] = back.astype(BF16)
        return carry

    for i in range(NCH // PAIR):
        last_loop(i, 0)
    pieces_sum(1)
    pieces_sum(0)
    leave(outb, fg_ref)
    for row, (sums, part) in enumerate(((sums1, 1), (sums1, 0), (sums2, 1), (sums2, 0))):
        ng_ref[row : row + 1, :] = sums[part : part + 1, 0:C] * total ** -0.5
    for e in range(NEXCH):
        sent_all(e)
        forwarded(e)
    pieces_out(1)
    pieces_out(0)


def finish(o_ref, fg_ref, dk1_ref, dk2_ref, ng_ref, *rest):
    outs, sem = rest[:-1], rest[-1]
    copies = [
        pltpu.make_async_copy(src, dst, sem.at[k])
        for k, (src, dst) in enumerate(zip((o_ref, fg_ref, dk1_ref, dk2_ref, ng_ref), outs))
    ]
    for copy in copies:
        copy.start()
    for copy in copies:
        copy.wait()


def local(features, kernel_one, gain_one, bias_one, kernel_two, gain_two, bias_two, cotangent):
    C, X, Y, Z = features.shape
    nx, ny = lax.axis_size("gx"), lax.axis_size("gy")
    n = nx * ny
    total = float(X * Y * Z * nx * ny)
    R = Z // 2
    NCH = Y // CH
    piece = -(-224 // (8 * n)) * 8
    taps = lambda k: jnp.transpose(k, (2, 3, 4, 0, 1)).reshape(27, C, C)
    row = lambda v: v.reshape(1, C)
    rows, all_rows = Y * R, (Y + 2) * R
    packed = CH * R // 2 + 16
    V = pltpu.VMEM
    DMA = pltpu.SemaphoreType.DMA
    scratch = [
        V((rows, L), F32), V((8, L), F32), V((R, 2 * Z), BF16), V((2 * L, 2 * Z), BF16),
        V((L, L), BF16), V((27, C, L), F32),
    ]
    scratch += [V((3, 2 * L, 2 * L), BF16)] * 4
    scratch += [V((all_rows, L), BF16)] * 8
    scratch += [V((2 * L, rows), BF16)] * 2
    scratch += [V((rows, L), F32)] * 2
    scratch += [V((all_rows, L), F32)] * 7
    scratch += [
        V((rows, L), BF16), V((2 * CH, R + 16, L), F32), V((NCH, L), F32), V((NCH, L), F32),
        V((NCH, L), F32), V((3, 2 * L, 2 * L), F32),
    ]
    scratch += [V((NEXCH, NCH, packed, L), BF16)] * 2 + [V((NEXCH, 3, R + 16, L), BF16)]
    scratch += [V((NEXCH, NCH, packed, L), BF16)] * 2 + [V((NEXCH, 2, R + 16, L), BF16)] * 3
    scratch += [DMA((NEXCH, 2 * NCH + 6))] * 2
    scratch += [V((4, 2, L), F32), V((4, n, 2, L), F32), DMA((4,)), DMA((4,))]
    scratch += [
        V((2, n, piece, L), F32), V((2, n, piece, L), F32), V((2, piece, L), BF16),
        V((2, n, piece, L), BF16), DMA((2, 2)), DMA((2, 2)),
        V((C, X, Y, Z), BF16), V((C, X, Y, Z), BF16), V((27, C, C), BF16), V((27, C, C), BF16),
        *[V((1, C), F32)] * 4, DMA((8,)), V((NEXCH, NCH // 2, packed, L), BF16),
        DMA((NEXCH, NCH // 2)), DMA((NEXCH, NCH // 2)),
    ]
    vmem = pl.BlockSpec(memory_space=pltpu.VMEM)
    anywhere = pl.BlockSpec(memory_space=pl.ANY)
    terms = jax.ShapeDtypeStruct((27, C, C), F32)
    volume = jax.ShapeDtypeStruct((C, X, Y, Z), BF16)
    mids = pl.pallas_call(
        functools.partial(kernel, nx, ny, total),
        name="blocks",
        out_shape=[
            volume, volume, terms, terms, jax.ShapeDtypeStruct((4, C), F32),
        ],
        in_specs=[pl.BlockSpec(memory_space=pltpu.HBM)] * 8,
        out_specs=[vmem] * 5,
        scratch_shapes=scratch,
        compiler_params=pltpu.CompilerParams(
            collective_id=0, has_side_effects=True, vmem_limit_bytes=48 << 20
        ),
    )(
        *[
            pltpu.with_memory_space_constraint(v, pltpu.HBM)
            for v in (
                features, cotangent, taps(kernel_one), taps(kernel_two),
                row(gain_one), row(bias_one), row(gain_two), row(bias_two),
            )
        ]
    )
    out, fg, dk1, dk2, norm = pl.pallas_call(
        finish,
        name="finish",
        out_shape=[volume, volume, terms, terms, jax.ShapeDtypeStruct((4, C), F32)],
        in_specs=[anywhere] * 5,
        out_specs=[anywhere] * 5,
        scratch_shapes=[DMA((5,))],
        compiler_params=pltpu.CompilerParams(vmem_limit_bytes=8 << 20),
    )(*mids)
    spatial = lambda d: jnp.transpose(d.reshape(3, 3, 3, C, C), (3, 4, 0, 1, 2))
    return out, fg, spatial(dk1), spatial(dk2), norm


def solution(mesh):
    in_specs = (P(None, "gx", "gy", None), P(), P(), P(), P(), P(), P(), P(None, "gx", "gy", None))
    out_specs = (P(None, "gx", "gy", None), P(None, "gx", "gy", None), P(), P(), P())
    return jax.shard_map(local, mesh=mesh, in_specs=in_specs, out_specs=out_specs, check_vma=False)
```

```python
import functools

import jax
import jax.numpy as jnp
from jax import lax
from jax.experimental import pallas as pl
from jax.experimental.pallas import tpu as pltpu
from jax.sharding import PartitionSpec as P

EPSILON = 1e-05
SLOPE = 0.01
SHARPNESS = 8.0
MESH = pl.DeviceIdType.MESH
LOGICAL = pl.DeviceIdType.LOGICAL
F32 = jnp.float32
BF16 = jnp.bfloat16
L = 128
CH = 4
FEAT, COT, HID1, HID2, SLO1 = range(5)
NEXCH = 5
NT = (((1,), (1,)), ((), ()))


def activate(s):
    scaled = SHARPNESS * s
    soft = jnp.maximum(scaled, 0.0) + jnp.log(1.0 + jnp.exp(-jnp.abs(scaled)))
    return SLOPE * s + ((1.0 - SLOPE) / SHARPNESS) * soft


def activate_slope(s):
    half = 0.5 * (1.0 - SLOPE)
    return (SLOPE + half) + half * jnp.tanh((0.5 * SHARPNESS) * s)


def untap(flat, out_ref, scale):
    C = out_ref.shape[1]
    for group in range(7):
        tall = jnp.transpose(flat[group * C : (group + 1) * C].astype(F32)) * scale
        for slot in range(min(4, 27 - 4 * group)):
            out_ref[4 * group + slot] = tall[slot * C : (slot + 1) * C]


def kernel(
    nx, ny, total,
    f_hbm, c_hbm, k1_hbm, k2_hbm, g1_hbm, b1_hbm, g2_hbm, b2_hbm,
    o_ref, fg_ref, dk1_ref, dk2_ref, ng_ref,
    t1, par, e_mat, s_mat, i_mat, base, wf1, wf2, wb2, wb1,
    vo_f, vh_f, vo_c, vh_c, vo_a, vh_a, vo_g, vh_g, vt_f, vt_a,
    hc1, hc2, n1o, n1h, n2o, n2h, s2o, s2h, s1o, outb, bs, mcs, scs, mcs1, raw,
    spr, spl, se, rl, rr, re, rdl, rdr, hs_sem, hr_sem,
    msg, st, ss_sem, sr_sem,
    pk, rsb, ags, agb, ws_sem, wr_sem,
    f_ref, c_ref, k1_ref, k2_ref, g1_ref, b1_ref, g2_ref, b2_ref, in_sem, rel, rel_sem, fwd_sem,
):
    C, X, Y, Z = f_ref.shape
    R = Z // 2
    CR = CH * R
    NCH = Y // CH
    n = nx * ny
    PIECE = rsb.shape[2]
    gx, gy = lax.axis_index("gx"), lax.axis_index("gy")
    me = gx * ny + gy
    has_l, has_r = gx > 0, gx < nx - 1
    has_d, has_u = gy > 0, gy < ny - 1

    def peer(k):
        other = me + k
        return jnp.where(other >= n, other - n, other)

    def others(use):
        if n & (n - 1):
            lax.fori_loop(1, n, lambda k, carry: (use(peer(k)), carry)[1], 0)
            return
        for dy in range(ny - 1, -1, -1):
            def body(t, carry, dy=dy):
                use(jnp.bitwise_xor(me, (nx - 1 - t) * ny + dy))
                return carry

            lax.fori_loop(0, nx if dy else nx - 1, body, 0)

    fetch = [
        pltpu.make_async_copy(src, dst, in_sem.at[k])
        for k, (src, dst) in enumerate(
            (
                (f_hbm, f_ref), (k1_hbm, k1_ref), (k2_hbm, k2_ref), (c_hbm, c_ref),
                (g1_hbm, g1_ref), (b1_hbm, b1_ref), (g2_hbm, g2_ref), (b2_hbm, b2_ref),
            )
        )
    ]
    for copy in fetch:
        copy.start()

    barrier = pltpu.get_barrier_semaphore()

    others(
        lambda d: pl.semaphore_signal(barrier, inc=1, device_id=d, device_id_type=LOGICAL)
    )

    lane = lax.broadcasted_iota(jnp.int32, (1, L), 1)
    xb = lax.rem(lane // C, 2) == 1
    z0 = lane < L // 2
    flag = lambda b: jnp.where(b, 1, 0)
    keep_h = jnp.where(xb, flag(has_l), flag(has_r)) > 0
    full_y = jnp.full((1, L), 1, jnp.int32)
    keep_o = [full_y * flag(has_d) > 0, full_y * flag(has_u) > 0]
    keep_ho = [(jnp.where(xb, flag(has_l), flag(has_r)) * flag(b)) > 0 for b in (has_d, has_u)]

    def row_of(y):
        return pl.multiple_of(y * R, R)

    def fold(v):
        v = v + pltpu.roll(v, C, 1)
        return v + pltpu.roll(v, 2 * C, 1)

    def loop(count, body, carry=0, unroll=1):
        def group(i, carry):
            for k in range(unroll):
                carry = body(i * unroll + k, carry)
            return carry

        return lax.fori_loop(0, count // unroll, group, carry)

    def eight(v):
        return jnp.sum(v.reshape(v.shape[0] // 8, 8, L), axis=0)

    def one(v):
        return jnp.sum(v, axis=0, keepdims=True)

    r_i = lax.broadcasted_iota(jnp.int32, (R, 2 * Z), 0)
    c_i = lax.broadcasted_iota(jnp.int32, (R, 2 * Z), 1)
    e_mat[...] = jnp.where(
        lax.rem(c_i, Z) == 2 * r_i + c_i // Z, 1.0, 0.0
    ).astype(BF16)
    r_i = lax.broadcasted_iota(jnp.int32, (2 * L, 2 * Z), 0)
    c_i = lax.broadcasted_iota(jnp.int32, (2 * L, 2 * Z), 1)
    same = lax.rem(r_i // R, 2) == c_i // Z
    s_mat[...] = jnp.where(
        same & (lax.rem(c_i, Z) == 2 * lax.rem(r_i, R) + r_i // L), 1.0, 0.0
    ).astype(BF16)
    r_i = lax.broadcasted_iota(jnp.int32, (L, L), 0)
    c_i = lax.broadcasted_iota(jnp.int32, (L, L), 1)
    i_mat[...] = jnp.where(r_i == c_i, 1.0, 0.0).astype(BF16)
    bs[...] = jnp.zeros(bs.shape, F32)

    spots_in = [(0, 0, z, x) for z in range(2) for x in range(2)]
    halo_x = {0: 2, 1: -1}
    rows_in = [(x, z) for _, _, z, x in spots_in] + [(halo_x[x], z) for _, _, z, x in spots_in]
    cols_a = [(x, z) for _, _, z, x in spots_in]
    cols_b = [(x, 2 if z == 0 else -1) for _, _, z, x in spots_in]

    def build(k_ref, w_ref, forward):
        if forward:
            stacked = jnp.concatenate([k_ref[t] for t in range(27) for _ in range(4)], axis=0)
            wide = lax.dot_general(
                i_mat[0:C, 0:C], stacked, NT, preferred_element_type=F32
            )
            for t in range(27):
                base[t] = wide[:, t * L : (t + 1) * L]
        else:
            r4 = lax.broadcasted_iota(jnp.int32, (C, L), 0)
            c4 = lax.rem(lax.broadcasted_iota(jnp.int32, (C, L), 1), C)
            spread4 = jnp.where(r4 == c4, 1.0, 0.0).astype(BF16)
            tall = k_ref[...].reshape(27 * C, C)
            wide = jnp.dot(tall, spread4, preferred_element_type=F32)
            for t in range(27):
                base[t] = wide[t * C : (t + 1) * C]
        block = lax.broadcasted_iota(jnp.int32, (C, L), 1) // C

        def one_row(j, carry):
            dy = j if forward else 2 - j
            for kb, (xi, zi) in enumerate(rows_in):
                for t, cols in enumerate((cols_a, cols_b)):
                    value = jnp.zeros((C, L), F32)
                    for b, (xo, zo) in enumerate(cols):
                        dx, dz = xi - xo + 1, zi - zo + 1
                        if not forward:
                            dx, dz = 2 - dx, 2 - dz
                        if 0 <= dx <= 2 and 0 <= dz <= 2:
                            tap = base[dx * 9 + dy * 3 + dz]
                            value = jnp.where(block == b, tap, value)
                    w_ref[j, kb * C : (kb + 1) * C, t * L : (t + 1) * L] = value.astype(BF16)
            return carry

        lax.fori_loop(0, 3, one_row, 0)

    def enter(in_ref, vo, e, after=None):
        def widen(c, carry):
            t1[pl.ds(pl.multiple_of(c * X * Y, X * Y), X * Y), :] = (
                in_ref[c].reshape(X * Y, Z).astype(F32)
            )
            return carry

        loop(C, widen, unroll=4)
        zero = jnp.zeros((X * C, Z), BF16)

        def chunk(c, carry):
            vs = []
            for k in range(CH):
                y = c * CH + k
                x0 = t1[pl.ds(y, C, stride=X * Y), :]
                x1 = t1[pl.ds(Y + y, C, stride=X * Y), :]
                xy = jnp.concatenate([x0, x1], axis=0).astype(BF16)
                rhs = jnp.concatenate(
                    [jnp.concatenate([xy, zero], axis=1), jnp.concatenate([zero, xy], axis=1)],
                    axis=0,
                )
                v = lax.dot_general(e_mat[...], rhs, NT, preferred_element_type=F32)
                vo[pl.ds(row_of(y + 1), R), :] = v.astype(BF16)
                vs.append(v)
            pack(e, c, vs, None)
            return carry

        for part in range(2):
            lax.fori_loop(
                part * NCH // 4, (part + 1) * NCH // 4,
                lambda h, carry: chunk(2 * h + 1, chunk(2 * h, carry)), 0,
            )
            if after is not None:
                after(part)

    def leave(src, dst):
        def pair(p, carry):
            o = src[pl.ds(pl.multiple_of(p * L, L), L), :]
            d = lax.dot_general(i_mat[...], o, NT, preferred_element_type=F32).astype(BF16)
            both = jnp.concatenate([d[: L // 2], d[L // 2 :]], axis=1)
            xs = jnp.dot(both, s_mat[...], preferred_element_type=F32)
            r0 = pl.multiple_of(p * 2 * R, 2 * R)
            t1[pl.ds(r0, R), :] = xs[:, :Z]
            t1[pl.ds(r0 + R, R), :] = xs[:, Z:]
            return carry

        with jax.named_scope("leave_pairs"):
            loop(Y // 2, pair, unroll=4)

        def channel(c, carry):
            for x in range(X):
                dst[c, x] = t1[pl.ds(x * C + c, Y, stride=X * C), :].astype(BF16)
            return carry

        with jax.named_scope("leave_channels"):
            loop(C, channel, unroll=4)

    def flip(vo, vt):
        def pair(p, carry):
            rows = vo[pl.ds(row_of(2 * p + 1), 2 * R), :]
            wide = rows.astype(F32)
            slot = 2 * lax.rem(p, 4)
            for k in range(2):
                bs[slot + k, 8 : 8 + R, :] = wide[k * R : (k + 1) * R]
            shifted = jnp.concatenate(
                [jnp.where(z0, bs[slot + k, 9 : 9 + R, :], bs[slot + k, 7 : 7 + R, :]) for k in range(2)],
                axis=0,
            ).astype(BF16)
            cols = pl.ds(pl.multiple_of(p * 2 * R, 2 * R), 2 * R)
            for k, part in enumerate((rows, shifted)):
                vt[k * L : (k + 1) * L, cols] = lax.dot_general(
                    i_mat[...], part, NT, preferred_element_type=F32
                ).astype(BF16)
            return carry

        loop(Y // 2, pair, unroll=4)

    half = CR // 2

    def pair_rows(e, p):
        low = p * (R + centre_rows(e))
        return slice(low, low + R)

    def centre_rows(e):
        return 0 if e in (FEAT, COT) else 16

    def pack(e, c, vs, center):
        for p in range(CH // 2):
            a, b = vs[2 * p], vs[2 * p + 1]
            rows = pair_rows(e, p)
            spr[e, c, rows, :] = jnp.where(xb, a, pltpu.roll(b, L - C, 1)).astype(BF16)
            spl[e, c, rows, :] = jnp.where(xb, pltpu.roll(b, C, 1), a).astype(BF16)
        if center is not None:
            center = center.astype(BF16)
            spr[e, c, R : R + 16, :] = center
            spl[e, c, R : R + 16, :] = center

        first = 2 if isinstance(c, int) and c else jnp.where(c == 0, 0, 2)
        se[e, first, 0:R, :] = vs[0].astype(BF16)
        if center is not None:
            se[e, first, R : R + 16, :] = center
        last = jnp.where(c == NCH - 1, 1, 2)
        se[e, last, 0:R, :] = vs[CH - 1].astype(BF16)
        if center is not None:
            se[e, last, R : R + 16, :] = center

    def copy_of(e, index, src, dst, dx, dy):
        return lambda: pltpu.make_async_remote_copy(
            src_ref=src, dst_ref=dst,
            send_sem=hs_sem.at[e, index], recv_sem=hr_sem.at[e, index],
            device_id=(lax.rem(gx + dx + nx, nx), lax.rem(gy + dy + ny, ny)),
            device_id_type=MESH,
        )

    def used(e, ref, c):
        return ref.at[e, c, pl.ds(0, half + centre_rows(e))]

    def side_copies(e, c):
        return [
            (has_r, has_l, copy_of(e, c, used(e, spr, c), used(e, rl, c), 1, 0)),
            (has_l, has_r, copy_of(e, NCH + c, used(e, spl, c), used(e, rr, c), -1, 0)),
        ]

    def end_copies(e):
        size = R + centre_rows(e)
        end, low, high = pl.ds(0, size), pl.ds(0, size), pl.ds(R, size)
        both = jnp.logical_and
        m = 2 * NCH
        last = NCH - 1
        return [
            [
                (has_d, has_u, copy_of(e, m, se.at[e, 0, end], re.at[e, 1, end], 0, -1)),
                (both(has_r, has_d), both(has_l, has_u),
                 copy_of(e, m + 2, spr.at[e, 0, low], rdl.at[e, 1, end], 1, -1)),
                (both(has_l, has_d), both(has_r, has_u),
                 copy_of(e, m + 4, spl.at[e, 0, low], rdr.at[e, 1, end], -1, -1)),
            ],
            [
                (has_u, has_d, copy_of(e, m + 1, se.at[e, 1, end], re.at[e, 0, end], 0, 1)),
                (both(has_r, has_u), both(has_l, has_d),
                 copy_of(e, m + 3, spr.at[e, last, high], rdl.at[e, 0, end], 1, 1)),
                (both(has_l, has_u), both(has_r, has_d),
                 copy_of(e, m + 5, spl.at[e, last, high], rdr.at[e, 0, end], -1, 1)),
            ],
        ]

    def start(copies):
        for sends, _, copy in copies:
            @pl.when(sends)
            def _(copy=copy):
                copy().start()

    def arrive(copies):
        for _, takes, copy in copies:
            @pl.when(takes)
            def _(copy=copy):
                copy().wait_recv()

    RELAY = nx == 8
    HALF = range(NCH // 2)
    low_mid, high_mid = nx // 2 - 1, nx // 2

    def hop(e, h, src, dst, there, s_sem, r_sem):
        return pltpu.make_async_remote_copy(
            src_ref=src, dst_ref=dst, send_sem=s_sem, recv_sem=r_sem,
            device_id=(there, gy), device_id_type=MESH,
        )

    def send_early(e, c):
        h = c
        (_, _, right), (_, _, left) = side_copies(e, c)
        relays = (
            (gx == low_mid, has_r, right, spr, nx - 1, hs_sem.at[e, c]),
            (gx == high_mid, has_l, left, spl, 0, hs_sem.at[e, NCH + c]),
        )
        for via, sends, direct, src, there, s_sem in relays:
            @pl.when(via)
            def _(src=src, there=there, s_sem=s_sem):
                hop(e, h, used(e, src, c), used(e, rel, h), there, s_sem, rel_sem.at[e, h]).start()

            @pl.when(jnp.logical_and(sends, jnp.logical_not(via)))
            def _(direct=direct):
                direct().start()

    def forwards(e, h):
        c = h
        return (
            (gx == nx - 1, hop(e, h, used(e, rel, h), used(e, rl, c), high_mid, fwd_sem.at[e, h], hr_sem.at[e, c])),
            (gx == 0, hop(e, h, used(e, rel, h), used(e, rr, c), low_mid, fwd_sem.at[e, h], hr_sem.at[e, NCH + c])),
        ) if RELAY else ()

    def relay_arrives(e, h):
        hop(e, h, used(e, rel, h), used(e, rel, h), low_mid, fwd_sem.at[e, h], rel_sem.at[e, h]).wait_recv()

    def forward(e, which):
        for h in which:
            for here, copy in forwards(e, h):
                @pl.when(here)
                def _(h=h, copy=copy):
                    relay_arrives(e, h)
                    copy.start()

    def forwarded(e):
        for h in HALF:
            for here, copy in forwards(e, h):
                @pl.when(here)
                def _(copy=copy):
                    copy.wait_send()

    def send(e, c, early):
        if RELAY and early:
            send_early(e, c)
        else:
            start(side_copies(e, c))

    def send_ends(e):
        for copies in end_copies(e):
            start(copies)

    def send_part(e, part):
        def body(c, carry):
            send(e, c, part == 0)
            return carry

        lax.fori_loop(part * (NCH // 2), (part + 1) * (NCH // 2), body, 0)

    def send_all(e):
        send_part(e, 0)
        send_part(e, 1)
        send_ends(e)

    def arrive_ends(e):
        for copies in end_copies(e):
            arrive(copies)

    def arrive_all(e):
        def body(c, carry):
            arrive(side_copies(e, c))
            return carry

        lax.fori_loop(0, NCH, body, 0)
        arrive_ends(e)

    def sent_all(e):
        def done(copies):
            for sends, _, copy in copies:
                @pl.when(sends)
                def _(copy=copy):
                    copy().wait_send()

        def body(c, carry):
            done(side_copies(e, c))
            return carry

        lax.fori_loop(0, NCH, body, 0)
        for copies in end_copies(e):
            done(copies)

    def center_of(tile):
        wide = tile.astype(F32)
        return (wide[0:8] + wide[8:16])[0:1]

    def halo_rows(e, c):
        center = None
        if centre_rows(e):
            tile = slice(R, R + 16)
            center = jnp.where(xb, center_of(rl[e, c, tile, :]), center_of(rr[e, c, tile, :]))
        found = []
        for p in range(CH // 2):
            rows = pair_rows(e, p)
            a, b = rl[e, c, rows, :].astype(F32), rr[e, c, rows, :].astype(F32)
            found.append(jnp.where(xb, a, b))
            found.append(jnp.where(xb, pltpu.roll(a, C, 1), pltpu.roll(b, L - C, 1)))
        return found, center

    def end_rows(e, side):
        own, own_center, center = re[e, side, 0:R, :].astype(F32), None, None
        data = slice(0, R)
        if centre_rows(e):
            own_center = center_of(re[e, side, R : R + 16, :])
            tile = slice(R, R + 16)
            if side == 0:
                data, tile = slice(16, 16 + R), slice(0, 16)
            center = jnp.where(xb, center_of(rdl[e, side, tile, :]), center_of(rdr[e, side, tile, :]))
        a, b = rdl[e, side, data, :].astype(F32), rdr[e, side, data, :].astype(F32)
        if side == 0:
            a, b = pltpu.roll(a, C, 1), pltpu.roll(b, L - C, 1)
        return own, own_center, jnp.where(xb, a, b), center

    END = (0, Y + 1)

    def each_halo(e, use_halo, use_own):
        def body(c, carry):
            found, center = halo_rows(e, c)
            for k, value in enumerate(found):
                use_halo(row_of(c * CH + k + 1), value, center, keep_h)
            return carry

        loop(NCH, body, unroll=2)
        each_end(e, use_halo, use_own)

    def each_end(e, use_halo, use_own):
        for side in range(2):
            own, own_center, value, center = end_rows(e, side)
            use_own(END[side] * R, own, own_center, keep_o[side])
            use_halo(END[side] * R, value, center, keep_ho[side])

    def stats_send(r, top, low):
        row = lax.broadcasted_iota(jnp.int32, (2, L), 0)
        both = jnp.where(row == 0, top, low)
        msg[r] = both
        st[r, me] = both

        others(
            lambda d: pltpu.make_async_remote_copy(
                src_ref=msg.at[r], dst_ref=st.at[r, me],
                send_sem=ss_sem.at[r], recv_sem=sr_sem.at[r],
                device_id=d, device_id_type=LOGICAL,
            ).start()
        )

    def stats_wait(r):
        rest = st.at[r, pl.ds(0, n - 1)]
        pltpu.make_async_remote_copy(
            src_ref=rest, dst_ref=rest, send_sem=ss_sem.at[r], recv_sem=sr_sem.at[r],
            device_id=peer(1), device_id_type=LOGICAL,
        ).wait()
        return jnp.sum(st[r], axis=0)

    def pieces_send(w, phase):
        others(
            lambda d: pltpu.make_async_remote_copy(
                src_ref=pk.at[w, d] if phase == 0 else ags.at[w],
                dst_ref=(rsb if phase == 0 else agb).at[w, me],
                send_sem=ws_sem.at[w, phase], recv_sem=wr_sem.at[w, phase],
                device_id=d, device_id_type=LOGICAL,
            ).start()
        )

    def pieces_wait(w, phase):
        rest = (rsb if phase == 0 else agb).at[w, pl.ds(0, n - 1)]
        pltpu.make_async_remote_copy(
            src_ref=rest, dst_ref=rest,
            send_sem=ws_sem.at[w, phase], recv_sem=wr_sem.at[w, phase],
            device_id=peer(1), device_id_type=LOGICAL,
        ).wait()

    def kernel_products(vt, vo, vh):
        for j in range(3):
            g = jnp.concatenate([vo[j * R : (j + Y) * R, :], vh[j * R : (j + Y) * R, :]], axis=1)
            raw[j] = jnp.dot(vt[...], g, preferred_element_type=F32)

    def kernel_terms(w):
        block = lax.broadcasted_iota(jnp.int32, (C, L), 1) // C
        rows_v = cols_a + cols_b
        groups = [jnp.zeros((C, L), F32) for _ in range(7)]
        for j in range(3):
            dy = 2 - j
            for dx in range(3):
                for dz in range(3):
                    tap = dx * 9 + dy * 3 + dz
                    group, slot = tap // 4, tap % 4
                    for kb, (xv, zv) in enumerate(rows_v):
                        for cb, (xg, zg) in enumerate(rows_in):
                            if kb >= 4 and zv == 2 and zg != 1:
                                continue
                            if kb >= 4 and zv == -1 and zg != 0:
                                continue
                            if xv - xg + 1 != dx or zv - zg + 1 != dz:
                                continue
                            t, b = cb // 4, cb % 4
                            part = raw[j, kb * C : (kb + 1) * C, t * L : (t + 1) * L]
                            if slot != b:
                                part = pltpu.roll(part, (slot - b) % 4 * C, 1)
                            groups[group] = groups[group] + jnp.where(block == slot, part, 0.0)
        flat = jnp.concatenate(groups, axis=0)
        rows = n * PIECE
        if rows > flat.shape[0]:
            flat = jnp.concatenate([flat, jnp.zeros((rows - flat.shape[0], L), F32)], axis=0)
        pk[w] = flat.reshape(n, PIECE, L)
        rsb[w, me] = pk[w, me]

    def pieces_sum(w):
        pieces_wait(w, 0)
        whole = jnp.sum(rsb[w], axis=0).astype(BF16)
        ags[w] = whole
        agb[w, me] = whole
        pieces_send(w, 1)

    dk_refs = (dk1_ref, dk2_ref)

    def pieces_out(w):
        pieces_wait(w, 1)
        untap(agb[w].reshape(n * PIECE, L), dk_refs[w], total ** -0.5)

    def conv_rows(vo, vh, w_ref, c, slot=0):
        parts = []
        for j in range(3):
            rows = pl.ds(row_of(c * CH + j), CR)
            parts += [vo[rows, :], vh[rows, :]]
        ab = jnp.dot(
            jnp.concatenate(parts, axis=1), w_ref[...].reshape(6 * L, 2 * L),
            preferred_element_type=F32,
        )
        for k in range(CH):
            bs[slot + k, 8 : 8 + R, :] = ab[k * R : (k + 1) * R, L:]
        return [
            ab[k * R : (k + 1) * R, :L]
            + jnp.where(z0, bs[slot + k, 7 : 7 + R, :], bs[slot + k, 9 : 9 + R, :])
            for k in range(CH)
        ]

    def totals(vs):
        return fold(one(functools.reduce(jnp.add, [eight(v) for v in vs])))

    def center_near(s):
        mean = s / (4.0 * CR)
        high = mean.astype(BF16).astype(F32)
        low = (mean - high).astype(BF16).astype(F32)
        tile = jnp.concatenate(
            [jnp.broadcast_to(high, (8, L)), jnp.broadcast_to(low, (8, L))], axis=0
        )
        return high + low, tile

    cells = float(X * Y * Z)
    zero8 = jnp.zeros((8, L), F32)
    PAIR = 2

    def paired(e, step, carry, before=None, after=None):
        def group(i, carry, first):
            inner, s = carry
            if before is not None:
                before(i)
            found = []
            for k in range(PAIR):
                inner, vs = step(i * PAIR + k, k * CH, inner)
                found.append((vs, totals(vs)))
            if after is not None:
                after(i)
            center, tile = center_near(found[0][1] if first else s)
            for k, (vs, s) in enumerate(found):
                c = i * PAIR + k
                centers_of[e][pl.ds(c, 1), :] = center
                scs[pl.ds(c, 1), :] = s
                inner = keep_chunk(e, c, vs, center, tile, inner)
            if e != HID2 and i < early_groups(e):
                for k in range(PAIR):
                    send(e, i * PAIR + k, i < EARLY)
            return inner, s

        carry = group(0, (carry, None), True)
        for i in range(1, NCH // PAIR):
            carry = group(i, carry, False)
        return carry[0]

    EARLY = NCH // PAIR // 2

    def early_groups(e):
        return max(EARLY, NCH // PAIR - 1) if e == SLO1 else EARLY

    def send_late(e):
        for i in range(early_groups(e), NCH // PAIR):
            for k in range(PAIR):
                send(e, i * PAIR + k, i < EARLY)
        send_ends(e)

    centers_of = {HID1: mcs1, HID2: mcs, SLO1: mcs}

    def keep_chunk(e, c, vs, center, tile, inner):
        vs = [v - center for v in vs]
        pack(e, c, vs, tile)
        if e != SLO1:
            hc = hc1 if e == HID1 else hc2
            for k, v in enumerate(vs):
                hc[pl.ds(row_of(c * CH + k), R), :] = v
                inner = inner + eight(v * v)
        return inner

    def forward_loop(vo, vh, w_ref, e, before=None, after=None):
        def step(c, slot, squares):
            return squares, conv_rows(vo, vh, w_ref, c, slot)

        squares = fold(one(paired(e, step, zero8, before, after)))
        centers = centers_of[e][...]
        mean = one(scs[...]) / cells
        off = centers - mean
        rest = scs[...] - (4.0 * CR) * centers
        spread = squares + one(off * (2.0 * rest + (4.0 * CR) * off))
        return mean, spread

    def moments(r):
        sums = stats_wait(r)
        center = sums[0:1] / n

        off = st[r] - center
        between = jnp.sum(off * off, axis=0)[0:1]
        variance = (sums[1:2] + cells * between) / total
        return center, lax.rsqrt(variance + EPSILON)

    fetch[0].wait()

    def send_f(part):
        if part == 0:
            pl.semaphore_wait(barrier, n - 1)
        send_part(FEAT, part)

    enter(f_ref, vo_f, FEAT, send_f)
    send_ends(FEAT)
    fetch[1].wait()
    build(k1_ref, wf1, True)
    fetch[2].wait()
    build(k2_ref, wf2, True)
    build(k2_ref, wb2, False)
    build(k1_ref, wb1, False)
    fetch[3].wait()
    forward(FEAT, HALF)
    enter(c_ref, vo_c, COT)

    def put_f(dst):
        def use(row, value, center, keep):
            dst[pl.ds(row, R), :] = jnp.where(keep, value, 0.0).astype(BF16)

        return use

    arrive_ends(FEAT)
    each_end(FEAT, put_f(vh_f), put_f(vo_f))

    def take_f(c):
        found, _ = halo_rows(FEAT, c)
        for k, value in enumerate(found):
            put_f(vh_f)(row_of(c * CH + k + 1), value, None, keep_h)

    arrive(side_copies(FEAT, 0))
    take_f(0)

    def before_f(i):
        for c in range(i * PAIR + 1, min(i * PAIR + PAIR + 1, NCH)):
            arrive(side_copies(FEAT, c))
            take_f(c)

    mean, spread = forward_loop(vo_f, vh_f, wf1, HID1, before_f)
    stats_send(0, mean, spread)
    send_late(HID1)
    for copy in fetch[4:]:
        copy.wait()
    par[...] = jnp.zeros(par.shape, F32)
    for row, ref in enumerate((g1_ref, b1_ref, g2_ref, b2_ref)):
        par[row : row + 1, 0:C] = ref[...]
    params = fold(par[...])
    gain1, bias1, gain2, bias2 = [params[r : r + 1] for r in range(4)]
    flip(vo_f, vt_f)
    forward(HID1, HALF)
    center, inv1 = moments(0)
    send_all(COT)
    arrive_all(HID1)

    def put_a(n_dst, v_dst, inv, gain, bias, center):
        def use(row, value, mid, keep):
            normed = (value + (mid - center)) * inv
            n_dst[pl.ds(row, R), :] = normed
            a = activate(normed * gain + bias)
            v_dst[pl.ds(row, R), :] = (a if keep is None else jnp.where(keep, a, 0.0)).astype(BF16)

        return use

    own_a = put_a(n1o, vo_a, inv1, gain1, bias1, center)

    halo_a = put_a(n1h, vh_a, inv1, gain1, bias1, center)

    def active_chunk(c):
        mid = mcs1[c : c + 1, :]
        for k in range(CH):
            own_a(row_of(c * CH + k + 1), hc1[pl.ds(row_of(c * CH + k), R), :], mid, None)
        found, mid = halo_rows(HID1, c)
        for k, value in enumerate(found):
            halo_a(row_of(c * CH + k + 1), value, mid, keep_h)

    def after_a(i):
        for c in range(PAIR * (i + 1) + 1, min(PAIR * (i + 2) + 1, NCH)):
            active_chunk(c)

    each_end(HID1, halo_a, own_a)
    for c in range(min(PAIR + 1, NCH)):
        active_chunk(c)

    mean, spread = forward_loop(vo_a, vh_a, wf2, HID2, after=after_a)
    stats_send(1, mean, spread)
    flip(vo_a, vt_a)
    forward(COT, HALF)
    send_all(HID2)
    center, inv2 = moments(1)

    def own_output(c, carry):
        plain, along = carry
        mid = mcs[pl.ds(c, 1), :]
        for k in range(CH):
            y = c * CH + k
            normed = (hc2[pl.ds(row_of(y), R), :] + (mid - center)) * inv2
            shifted = normed * gain2 + bias2
            outb[pl.ds(row_of(y), R), :] = activate(shifted).astype(BF16)
            rows = pl.ds(row_of(y + 1), R)
            slope = vo_c[rows, :].astype(F32) * activate_slope(shifted)
            n2o[rows, :] = normed
            s2o[rows, :] = slope
            plain = plain + eight(slope)
            along = along + eight(slope * normed)
        return plain, along

    plain, along = lax.fori_loop(0, NCH, own_output, (zero8, zero8))
    stats_send(2, fold(one(plain)), fold(one(along)))

    forward(HID2, HALF)
    leave(outb, o_ref)
    arrive_all(COT)
    arrive_all(HID2)

    def put_c(dst):
        def use(row, value, mid, keep):
            dst[pl.ds(row, R), :] = value.astype(BF16)

        return use

    each_halo(COT, put_c(vh_c), put_c(vo_c))

    def put_s(n_dst, s_dst, c_src):
        def use(row, value, mid, keep):
            rows = pl.ds(row, R)
            normed = (value + (mid - center)) * inv2
            n_dst[rows, :] = normed
            s_dst[rows, :] = c_src[rows, :].astype(F32) * activate_slope(normed * gain2 + bias2)

        return use

    each_halo(HID2, put_s(n2h, s2h, vh_c), put_s(n2o, s2o, vo_c))
    sums2 = stats_wait(2)

    def gradient(slope, normed, sums, factor):
        return factor * (slope - sums[0:1] / total - normed * (sums[1:2] / total))

    factor2 = gain2 * inv2

    def grad_rows(row, keep_own, keep_halo):
        rows = pl.ds(row, R)
        g = gradient(s2o[rows, :], n2o[rows, :], sums2, factor2)
        vo_g[rows, :] = (g if keep_own is None else jnp.where(keep_own, g, 0.0)).astype(BF16)
        g = gradient(s2h[rows, :], n2h[rows, :], sums2, factor2)
        vh_g[rows, :] = jnp.where(keep_halo, g, 0.0).astype(BF16)

    def grad_two(c):
        for k in range(CH):
            grad_rows(row_of(c * CH + k + 1), None, keep_h)

    def after_g(i):
        for c in range(PAIR * (i + 1) + 1, min(PAIR * (i + 2) + 1, NCH)):
            grad_two(c)

    for c in range(min(PAIR + 1, NCH)):
        grad_two(c)
    for side in range(2):
        grad_rows(END[side] * R, keep_o[side], keep_ho[side])

    def back_step(c, slot, carry):
        plain, along = carry
        slopes = []
        for k, back in enumerate(conv_rows(vo_g, vh_g, wb2, c, slot)):
            rows = pl.ds(row_of(c * CH + k + 1), R)
            normed = n1o[rows, :]
            slope = back * activate_slope(normed * gain1 + bias1)
            s1o[rows, :] = slope
            plain = plain + eight(slope)
            along = along + eight(slope * normed)
            slopes.append(slope)
        return (plain, along), slopes

    plain, along = paired(SLO1, back_step, (zero8, zero8), after=after_g)
    stats_send(3, fold(one(plain)), fold(one(along)))
    send_late(SLO1)
    kernel_products(vt_a, vo_g, vh_g)
    forward(SLO1, HALF)
    kernel_terms(1)
    sums1 = stats_wait(3)
    arrive_all(SLO1)
    pieces_send(1, 0)
    factor1 = gain1 * inv1

    def put_g(dst, normed_ref):
        def use(row, value, mid, keep):
            rows = pl.ds(row, R)
            g = gradient(value + mid, normed_ref[rows, :], sums1, factor1)
            dst[rows, :] = jnp.where(keep, g, 0.0).astype(BF16)

        return use

    def grad_one(c, carry):
        for k in range(CH):
            rows = pl.ds(row_of(c * CH + k + 1), R)
            vo_g[rows, :] = gradient(s1o[rows, :], n1o[rows, :], sums1, factor1).astype(BF16)
        return carry

    lax.fori_loop(0, NCH, grad_one, 0)
    each_halo(SLO1, put_g(vh_g, n1h), put_g(vo_g, n1o))
    kernel_products(vt_f, vo_g, vh_g)
    kernel_terms(0)
    pieces_send(0, 0)

    def last_loop(i, carry):
        for j in range(PAIR):
            c = i * PAIR + j
            for k, back in enumerate(conv_rows(vo_g, vh_g, wb1, c, j * CH)):
                outb[pl.ds(row_of(c * CH + k), R), :] = back.astype(BF16)
        return carry

    for i in range(NCH // PAIR):
        last_loop(i, 0)
    pieces_sum(1)
    pieces_sum(0)
    leave(outb, fg_ref)
    for row, (sums, part) in enumerate(((sums1, 1), (sums1, 0), (sums2, 1), (sums2, 0))):
        ng_ref[row : row + 1, :] = sums[part : part + 1, 0:C] * total ** -0.5
    for e in range(NEXCH):
        sent_all(e)
        forwarded(e)
    pieces_out(1)
    pieces_out(0)


def finish(o_ref, fg_ref, dk1_ref, dk2_ref, ng_ref, *rest):
    outs, sem = rest[:-1], rest[-1]
    copies = [
        pltpu.make_async_copy(src, dst, sem.at[k])
        for k, (src, dst) in enumerate(zip((o_ref, fg_ref, dk1_ref, dk2_ref, ng_ref), outs))
    ]
    for copy in copies:
        copy.start()
    for copy in copies:
        copy.wait()


def local(features, kernel_one, gain_one, bias_one, kernel_two, gain_two, bias_two, cotangent):
    C, X, Y, Z = features.shape
    nx, ny = lax.axis_size("gx"), lax.axis_size("gy")
    n = nx * ny
    total = float(X * Y * Z * nx * ny)
    R = Z // 2
    NCH = Y // CH
    piece = -(-224 // (8 * n)) * 8
    taps = lambda k: jnp.transpose(k, (2, 3, 4, 0, 1)).reshape(27, C, C)
    row = lambda v: v.reshape(1, C)
    rows, all_rows = Y * R, (Y + 2) * R
    packed = CH * R // 2 + 16
    V = pltpu.VMEM
    DMA = pltpu.SemaphoreType.DMA
    scratch = [
        V((rows, L), F32), V((8, L), F32), V((R, 2 * Z), BF16), V((2 * L, 2 * Z), BF16),
        V((L, L), BF16), V((27, C, L), F32),
    ]
    scratch += [V((3, 2 * L, 2 * L), BF16)] * 4
    scratch += [V((all_rows, L), BF16)] * 8
    scratch += [V((2 * L, rows), BF16)] * 2
    scratch += [V((rows, L), F32)] * 2
    scratch += [V((all_rows, L), F32)] * 7
    scratch += [
        V((rows, L), BF16), V((2 * CH, R + 16, L), F32), V((NCH, L), F32), V((NCH, L), F32),
        V((NCH, L), F32), V((3, 2 * L, 2 * L), F32),
    ]
    scratch += [V((NEXCH, NCH, packed, L), BF16)] * 2 + [V((NEXCH, 3, R + 16, L), BF16)]
    scratch += [V((NEXCH, NCH, packed, L), BF16)] * 2 + [V((NEXCH, 2, R + 16, L), BF16)] * 3
    scratch += [DMA((NEXCH, 2 * NCH + 6))] * 2
    scratch += [V((4, 2, L), F32), V((4, n, 2, L), F32), DMA((4,)), DMA((4,))]
    scratch += [
        V((2, n, piece, L), F32), V((2, n, piece, L), F32), V((2, piece, L), BF16),
        V((2, n, piece, L), BF16), DMA((2, 2)), DMA((2, 2)),
        V((C, X, Y, Z), BF16), V((C, X, Y, Z), BF16), V((27, C, C), BF16), V((27, C, C), BF16),
        *[V((1, C), F32)] * 4, DMA((8,)), V((NEXCH, NCH // 2, packed, L), BF16),
        DMA((NEXCH, NCH // 2)), DMA((NEXCH, NCH // 2)),
    ]
    vmem = pl.BlockSpec(memory_space=pltpu.VMEM)
    anywhere = pl.BlockSpec(memory_space=pl.ANY)
    terms = jax.ShapeDtypeStruct((27, C, C), F32)
    volume = jax.ShapeDtypeStruct((C, X, Y, Z), BF16)
    mids = pl.pallas_call(
        functools.partial(kernel, nx, ny, total),
        name="blocks",
        out_shape=[
            volume, volume, terms, terms, jax.ShapeDtypeStruct((4, C), F32),
        ],
        in_specs=[pl.BlockSpec(memory_space=pltpu.HBM)] * 8,
        out_specs=[vmem] * 5,
        scratch_shapes=scratch,
        compiler_params=pltpu.CompilerParams(
            collective_id=0, has_side_effects=True, vmem_limit_bytes=48 << 20
        ),
    )(
        *[
            pltpu.with_memory_space_constraint(v, pltpu.HBM)
            for v in (
                features, cotangent, taps(kernel_one), taps(kernel_two),
                row(gain_one), row(bias_one), row(gain_two), row(bias_two),
            )
        ]
    )
    out, fg, dk1, dk2, norm = pl.pallas_call(
        finish,
        name="finish",
        out_shape=[volume, volume, terms, terms, jax.ShapeDtypeStruct((4, C), F32)],
        in_specs=[anywhere] * 5,
        out_specs=[anywhere] * 5,
        scratch_shapes=[DMA((5,))],
        compiler_params=pltpu.CompilerParams(vmem_limit_bytes=8 << 20),
    )(*mids)
    spatial = lambda d: jnp.transpose(d.reshape(3, 3, 3, C, C), (3, 4, 0, 1, 2))
    return out, fg, spatial(dk1), spatial(dk2), norm


def solution(mesh):
    in_specs = (P(None, "gx", "gy", None), P(), P(), P(), P(), P(), P(), P(None, "gx", "gy", None))
    out_specs = (P(None, "gx", "gy", None), P(None, "gx", "gy", None), P(), P(), P())
    return jax.shard_map(local, mesh=mesh, in_specs=in_specs, out_specs=out_specs, check_vma=False)
```

```python
import functools

import jax
import jax.numpy as jnp
from jax import lax
from jax.experimental import pallas as pl
from jax.experimental.pallas import tpu as pltpu
from jax.sharding import PartitionSpec as P

EPSILON = 1e-05
SLOPE = 0.01
SHARPNESS = 8.0
MESH = pl.DeviceIdType.MESH
LOGICAL = pl.DeviceIdType.LOGICAL
F32 = jnp.float32
BF16 = jnp.bfloat16
L = 128
CH = 4
FEAT, COT, HID1, HID2, SLO1 = range(5)
NEXCH = 5
NT = (((1,), (1,)), ((), ()))


def activate(s):
    scaled = SHARPNESS * s
    soft = jnp.maximum(scaled, 0.0) + jnp.log(1.0 + jnp.exp(-jnp.abs(scaled)))
    return SLOPE * s + ((1.0 - SLOPE) / SHARPNESS) * soft


def activate_slope(s):
    half = 0.5 * (1.0 - SLOPE)
    return (SLOPE + half) + half * jnp.tanh((0.5 * SHARPNESS) * s)


def untap(flat, out_ref, scale):
    C = out_ref.shape[1]
    for group in range(7):
        tall = jnp.transpose(flat[group * C : (group + 1) * C].astype(F32)) * scale
        for slot in range(min(4, 27 - 4 * group)):
            out_ref[4 * group + slot] = tall[slot * C : (slot + 1) * C]


def kernel(
    nx, ny, total,
    f_hbm, c_hbm, k1_hbm, k2_hbm, g1_hbm, b1_hbm, g2_hbm, b2_hbm,
    o_ref, fg_ref, dk1_ref, dk2_ref, ng_ref,
    t1, par, e_mat, s_mat, i_mat, base, wf1, wf2, wb2, wb1,
    vo_f, vh_f, vo_c, vh_c, vo_a, vh_a, vo_g, vh_g, vt_f, vt_a,
    hc1, hc2, n1o, n1h, n2o, n2h, s2o, s2h, s1o, outb, bs, mcs, scs, mcs1, raw,
    spr, spl, se, rl, rr, re, rdl, rdr, hs_sem, hr_sem,
    msg, st, ss_sem, sr_sem,
    pk, rsb, ags, agb, ws_sem, wr_sem,
    f_ref, c_ref, k1_ref, k2_ref, g1_ref, b1_ref, g2_ref, b2_ref, in_sem, rel, rel_sem, fwd_sem,
):
    C, X, Y, Z = f_ref.shape
    R = Z // 2
    CR = CH * R
    NCH = Y // CH
    n = nx * ny
    PIECE = rsb.shape[2]
    gx, gy = lax.axis_index("gx"), lax.axis_index("gy")
    me = gx * ny + gy
    has_l, has_r = gx > 0, gx < nx - 1
    has_d, has_u = gy > 0, gy < ny - 1

    def peer(k):
        other = me + k
        return jnp.where(other >= n, other - n, other)

    def others(use):
        if n & (n - 1):
            lax.fori_loop(1, n, lambda k, carry: (use(peer(k)), carry)[1], 0)
            return
        for dy in range(ny - 1, -1, -1):
            def body(t, carry, dy=dy):
                use(jnp.bitwise_xor(me, (nx - 1 - t) * ny + dy))
                return carry

            lax.fori_loop(0, nx if dy else nx - 1, body, 0)

    fetch = [
        pltpu.make_async_copy(src, dst, in_sem.at[k])
        for k, (src, dst) in enumerate(
            (
                (f_hbm, f_ref), (k1_hbm, k1_ref), (k2_hbm, k2_ref), (c_hbm, c_ref),
                (g1_hbm, g1_ref), (b1_hbm, b1_ref), (g2_hbm, g2_ref), (b2_hbm, b2_ref),
            )
        )
    ]
    for copy in fetch:
        copy.start()

    barrier = pltpu.get_barrier_semaphore()

    others(
        lambda d: pl.semaphore_signal(barrier, inc=1, device_id=d, device_id_type=LOGICAL)
    )

    lane = lax.broadcasted_iota(jnp.int32, (1, L), 1)
    xb = lax.rem(lane // C, 2) == 1
    z0 = lane < L // 2
    flag = lambda b: jnp.where(b, 1, 0)
    keep_h = jnp.where(xb, flag(has_l), flag(has_r)) > 0
    full_y = jnp.full((1, L), 1, jnp.int32)
    keep_o = [full_y * flag(has_d) > 0, full_y * flag(has_u) > 0]
    keep_ho = [(jnp.where(xb, flag(has_l), flag(has_r)) * flag(b)) > 0 for b in (has_d, has_u)]

    def row_of(y):
        return pl.multiple_of(y * R, R)

    def fold(v):
        v = v + pltpu.roll(v, C, 1)
        return v + pltpu.roll(v, 2 * C, 1)

    def loop(count, body, carry=0, unroll=1):
        def group(i, carry):
            for k in range(unroll):
                carry = body(i * unroll + k, carry)
            return carry

        return lax.fori_loop(0, count // unroll, group, carry)

    def eight(v):
        return jnp.sum(v.reshape(v.shape[0] // 8, 8, L), axis=0)

    def one(v):
        return jnp.sum(v, axis=0, keepdims=True)

    r_i = lax.broadcasted_iota(jnp.int32, (R, 2 * Z), 0)
    c_i = lax.broadcasted_iota(jnp.int32, (R, 2 * Z), 1)
    e_mat[...] = jnp.where(
        lax.rem(c_i, Z) == 2 * r_i + c_i // Z, 1.0, 0.0
    ).astype(BF16)
    r_i = lax.broadcasted_iota(jnp.int32, (2 * L, 2 * Z), 0)
    c_i = lax.broadcasted_iota(jnp.int32, (2 * L, 2 * Z), 1)
    same = lax.rem(r_i // R, 2) == c_i // Z
    s_mat[...] = jnp.where(
        same & (lax.rem(c_i, Z) == 2 * lax.rem(r_i, R) + r_i // L), 1.0, 0.0
    ).astype(BF16)
    r_i = lax.broadcasted_iota(jnp.int32, (L, L), 0)
    c_i = lax.broadcasted_iota(jnp.int32, (L, L), 1)
    i_mat[...] = jnp.where(r_i == c_i, 1.0, 0.0).astype(BF16)
    bs[...] = jnp.zeros(bs.shape, F32)

    spots_in = [(0, 0, z, x) for z in range(2) for x in range(2)]
    halo_x = {0: 2, 1: -1}
    rows_in = [(x, z) for _, _, z, x in spots_in] + [(halo_x[x], z) for _, _, z, x in spots_in]
    cols_a = [(x, z) for _, _, z, x in spots_in]
    cols_b = [(x, 2 if z == 0 else -1) for _, _, z, x in spots_in]

    def build(k_ref, w_ref, forward):
        if forward:
            stacked = jnp.concatenate([k_ref[t] for t in range(27) for _ in range(4)], axis=0)
            wide = lax.dot_general(
                i_mat[0:C, 0:C], stacked, NT, preferred_element_type=F32
            )
            for t in range(27):
                base[t] = wide[:, t * L : (t + 1) * L]
        else:
            r4 = lax.broadcasted_iota(jnp.int32, (C, L), 0)
            c4 = lax.rem(lax.broadcasted_iota(jnp.int32, (C, L), 1), C)
            spread4 = jnp.where(r4 == c4, 1.0, 0.0).astype(BF16)
            tall = k_ref[...].reshape(27 * C, C)
            wide = jnp.dot(tall, spread4, preferred_element_type=F32)
            for t in range(27):
                base[t] = wide[t * C : (t + 1) * C]
        block = lax.broadcasted_iota(jnp.int32, (C, L), 1) // C

        def one_row(j, carry):
            dy = j if forward else 2 - j
            for kb, (xi, zi) in enumerate(rows_in):
                for t, cols in enumerate((cols_a, cols_b)):
                    value = jnp.zeros((C, L), F32)
                    for b, (xo, zo) in enumerate(cols):
                        dx, dz = xi - xo + 1, zi - zo + 1
                        if not forward:
                            dx, dz = 2 - dx, 2 - dz
                        if 0 <= dx <= 2 and 0 <= dz <= 2:
                            tap = base[dx * 9 + dy * 3 + dz]
                            value = jnp.where(block == b, tap, value)
                    w_ref[j, kb * C : (kb + 1) * C, t * L : (t + 1) * L] = value.astype(BF16)
            return carry

        lax.fori_loop(0, 3, one_row, 0)

    def enter(in_ref, vo, e, after=None):
        def widen(c, carry):
            t1[pl.ds(pl.multiple_of(c * X * Y, X * Y), X * Y), :] = (
                in_ref[c].reshape(X * Y, Z).astype(F32)
            )
            return carry

        loop(C, widen, unroll=4)
        zero = jnp.zeros((X * C, Z), BF16)

        def chunk(c, carry):
            vs = []
            for k in range(CH):
                y = c * CH + k
                x0 = t1[pl.ds(y, C, stride=X * Y), :]
                x1 = t1[pl.ds(Y + y, C, stride=X * Y), :]
                xy = jnp.concatenate([x0, x1], axis=0).astype(BF16)
                rhs = jnp.concatenate(
                    [jnp.concatenate([xy, zero], axis=1), jnp.concatenate([zero, xy], axis=1)],
                    axis=0,
                )
                v = lax.dot_general(e_mat[...], rhs, NT, preferred_element_type=F32)
                vo[pl.ds(row_of(y + 1), R), :] = v.astype(BF16)
                vs.append(v)
            pack(e, c, vs, None)
            return carry

        for part in range(2):
            lax.fori_loop(
                part * NCH // 4, (part + 1) * NCH // 4,
                lambda h, carry: chunk(2 * h + 1, chunk(2 * h, carry)), 0,
            )
            if after is not None:
                after(part)

    def leave(src, dst):
        def pair(p, carry):
            o = src[pl.ds(pl.multiple_of(p * L, L), L), :]
            d = lax.dot_general(i_mat[...], o, NT, preferred_element_type=F32).astype(BF16)
            both = jnp.concatenate([d[: L // 2], d[L // 2 :]], axis=1)
            xs = jnp.dot(both, s_mat[...], preferred_element_type=F32)
            r0 = pl.multiple_of(p * 2 * R, 2 * R)
            t1[pl.ds(r0, R), :] = xs[:, :Z]
            t1[pl.ds(r0 + R, R), :] = xs[:, Z:]
            return carry

        with jax.named_scope("leave_pairs"):
            loop(Y // 2, pair, unroll=4)

        def channel(c, carry):
            for x in range(X):
                dst[c, x] = t1[pl.ds(x * C + c, Y, stride=X * C), :].astype(BF16)
            return carry

        with jax.named_scope("leave_channels"):
            loop(C, channel, unroll=4)

    def flip(vo, vt):
        def pair(p, carry):
            rows = vo[pl.ds(row_of(2 * p + 1), 2 * R), :]
            wide = rows.astype(F32)
            slot = 2 * lax.rem(p, 4)
            for k in range(2):
                bs[slot + k, 8 : 8 + R, :] = wide[k * R : (k + 1) * R]
            shifted = jnp.concatenate(
                [jnp.where(z0, bs[slot + k, 9 : 9 + R, :], bs[slot + k, 7 : 7 + R, :]) for k in range(2)],
                axis=0,
            ).astype(BF16)
            cols = pl.ds(pl.multiple_of(p * 2 * R, 2 * R), 2 * R)
            for k, part in enumerate((rows, shifted)):
                vt[k * L : (k + 1) * L, cols] = lax.dot_general(
                    i_mat[...], part, NT, preferred_element_type=F32
                ).astype(BF16)
            return carry

        loop(Y // 2, pair, unroll=4)

    half = CR // 2

    def pair_rows(e, p):
        low = p * (R + centre_rows(e))
        return slice(low, low + R)

    def centre_rows(e):
        return 0 if e in (FEAT, COT) else 16

    def pack(e, c, vs, center):
        for p in range(CH // 2):
            a, b = vs[2 * p], vs[2 * p + 1]
            rows = pair_rows(e, p)
            spr[e, c, rows, :] = jnp.where(xb, a, pltpu.roll(b, L - C, 1)).astype(BF16)
            spl[e, c, rows, :] = jnp.where(xb, pltpu.roll(b, C, 1), a).astype(BF16)
        if center is not None:
            center = center.astype(BF16)
            spr[e, c, R : R + 16, :] = center
            spl[e, c, R : R + 16, :] = center

        first = 2 if isinstance(c, int) and c else jnp.where(c == 0, 0, 2)
        se[e, first, 0:R, :] = vs[0].astype(BF16)
        if center is not None:
            se[e, first, R : R + 16, :] = center
        last = jnp.where(c == NCH - 1, 1, 2)
        se[e, last, 0:R, :] = vs[CH - 1].astype(BF16)
        if center is not None:
            se[e, last, R : R + 16, :] = center

    def copy_of(e, index, src, dst, dx, dy):
        return lambda: pltpu.make_async_remote_copy(
            src_ref=src, dst_ref=dst,
            send_sem=hs_sem.at[e, index], recv_sem=hr_sem.at[e, index],
            device_id=(lax.rem(gx + dx + nx, nx), lax.rem(gy + dy + ny, ny)),
            device_id_type=MESH,
        )

    def used(e, ref, c):
        return ref.at[e, c, pl.ds(0, half + centre_rows(e))]

    def side_copies(e, c):
        return [
            (has_r, has_l, copy_of(e, c, used(e, spr, c), used(e, rl, c), 1, 0)),
            (has_l, has_r, copy_of(e, NCH + c, used(e, spl, c), used(e, rr, c), -1, 0)),
        ]

    def end_copies(e):
        size = R + centre_rows(e)
        end, low, high = pl.ds(0, size), pl.ds(0, size), pl.ds(R, size)
        both = jnp.logical_and
        m = 2 * NCH
        last = NCH - 1
        return [
            [
                (has_d, has_u, copy_of(e, m, se.at[e, 0, end], re.at[e, 1, end], 0, -1)),
                (both(has_r, has_d), both(has_l, has_u),
                 copy_of(e, m + 2, spr.at[e, 0, low], rdl.at[e, 1, end], 1, -1)),
                (both(has_l, has_d), both(has_r, has_u),
                 copy_of(e, m + 4, spl.at[e, 0, low], rdr.at[e, 1, end], -1, -1)),
            ],
            [
                (has_u, has_d, copy_of(e, m + 1, se.at[e, 1, end], re.at[e, 0, end], 0, 1)),
                (both(has_r, has_u), both(has_l, has_d),
                 copy_of(e, m + 3, spr.at[e, last, high], rdl.at[e, 0, end], 1, 1)),
                (both(has_l, has_u), both(has_r, has_d),
                 copy_of(e, m + 5, spl.at[e, last, high], rdr.at[e, 0, end], -1, 1)),
            ],
        ]

    def start(copies):
        for sends, _, copy in copies:
            @pl.when(sends)
            def _(copy=copy):
                copy().start()

    def arrive(copies):
        for _, takes, copy in copies:
            @pl.when(takes)
            def _(copy=copy):
                copy().wait_recv()

    RELAY = nx == 8
    HALF = range(NCH // 2)
    low_mid, high_mid = nx // 2 - 1, nx // 2

    def hop(e, h, src, dst, there, s_sem, r_sem):
        return pltpu.make_async_remote_copy(
            src_ref=src, dst_ref=dst, send_sem=s_sem, recv_sem=r_sem,
            device_id=(there, gy), device_id_type=MESH,
        )

    def send_early(e, c):
        h = c
        (_, _, right), (_, _, left) = side_copies(e, c)
        relays = (
            (gx == low_mid, has_r, right, spr, nx - 1, hs_sem.at[e, c]),
            (gx == high_mid, has_l, left, spl, 0, hs_sem.at[e, NCH + c]),
        )
        for via, sends, direct, src, there, s_sem in relays:
            @pl.when(via)
            def _(src=src, there=there, s_sem=s_sem):
                hop(e, h, used(e, src, c), used(e, rel, h), there, s_sem, rel_sem.at[e, h]).start()

            @pl.when(jnp.logical_and(sends, jnp.logical_not(via)))
            def _(direct=direct):
                direct().start()

    def forwards(e, h):
        c = h
        return (
            (gx == nx - 1, hop(e, h, used(e, rel, h), used(e, rl, c), high_mid, fwd_sem.at[e, h], hr_sem.at[e, c])),
            (gx == 0, hop(e, h, used(e, rel, h), used(e, rr, c), low_mid, fwd_sem.at[e, h], hr_sem.at[e, NCH + c])),
        ) if RELAY else ()

    def relay_arrives(e, h):
        hop(e, h, used(e, rel, h), used(e, rel, h), low_mid, fwd_sem.at[e, h], rel_sem.at[e, h]).wait_recv()

    def forward(e, which):
        for h in which:
            for here, copy in forwards(e, h):
                @pl.when(here)
                def _(h=h, copy=copy):
                    relay_arrives(e, h)
                    copy.start()

    def forwarded(e):
        for h in HALF:
            for here, copy in forwards(e, h):
                @pl.when(here)
                def _(copy=copy):
                    copy.wait_send()

    def send(e, c, early):
        if RELAY and early:
            send_early(e, c)
        else:
            start(side_copies(e, c))

    def send_ends(e):
        for copies in end_copies(e):
            start(copies)

    def send_part(e, part):
        def body(c, carry):
            send(e, c, part == 0)
            return carry

        lax.fori_loop(part * (NCH // 2), (part + 1) * (NCH // 2), body, 0)

    def send_all(e):
        send_part(e, 0)
        send_part(e, 1)
        send_ends(e)

    def arrive_ends(e):
        for copies in end_copies(e):
            arrive(copies)

    def arrive_all(e):
        def body(c, carry):
            arrive(side_copies(e, c))
            return carry

        lax.fori_loop(0, NCH, body, 0)
        arrive_ends(e)

    def sent_all(e):
        def done(copies):
            for sends, _, copy in copies:
                @pl.when(sends)
                def _(copy=copy):
                    copy().wait_send()

        def body(c, carry):
            done(side_copies(e, c))
            return carry

        lax.fori_loop(0, NCH, body, 0)
        for copies in end_copies(e):
            done(copies)

    def center_of(tile):
        wide = tile.astype(F32)
        return (wide[0:8] + wide[8:16])[0:1]

    def halo_rows(e, c):
        center = None
        if centre_rows(e):
            tile = slice(R, R + 16)
            center = jnp.where(xb, center_of(rl[e, c, tile, :]), center_of(rr[e, c, tile, :]))
        found = []
        for p in range(CH // 2):
            rows = pair_rows(e, p)
            a, b = rl[e, c, rows, :].astype(F32), rr[e, c, rows, :].astype(F32)
            found.append(jnp.where(xb, a, b))
            found.append(jnp.where(xb, pltpu.roll(a, C, 1), pltpu.roll(b, L - C, 1)))
        return found, center

    def end_rows(e, side):
        own, own_center, center = re[e, side, 0:R, :].astype(F32), None, None
        data = slice(0, R)
        if centre_rows(e):
            own_center = center_of(re[e, side, R : R + 16, :])
            tile = slice(R, R + 16)
            if side == 0:
                data, tile = slice(16, 16 + R), slice(0, 16)
            center = jnp.where(xb, center_of(rdl[e, side, tile, :]), center_of(rdr[e, side, tile, :]))
        a, b = rdl[e, side, data, :].astype(F32), rdr[e, side, data, :].astype(F32)
        if side == 0:
            a, b = pltpu.roll(a, C, 1), pltpu.roll(b, L - C, 1)
        return own, own_center, jnp.where(xb, a, b), center

    END = (0, Y + 1)

    def each_halo(e, use_halo, use_own):
        def body(c, carry):
            found, center = halo_rows(e, c)
            for k, value in enumerate(found):
                use_halo(row_of(c * CH + k + 1), value, center, keep_h)
            return carry

        loop(NCH, body, unroll=2)
        each_end(e, use_halo, use_own)

    def each_end(e, use_halo, use_own):
        for side in range(2):
            own, own_center, value, center = end_rows(e, side)
            use_own(END[side] * R, own, own_center, keep_o[side])
            use_halo(END[side] * R, value, center, keep_ho[side])

    def stats_send(r, top, low):
        row = lax.broadcasted_iota(jnp.int32, (2, L), 0)
        both = jnp.where(row == 0, top, low)
        msg[r] = both
        st[r, me] = both

        others(
            lambda d: pltpu.make_async_remote_copy(
                src_ref=msg.at[r], dst_ref=st.at[r, me],
                send_sem=ss_sem.at[r], recv_sem=sr_sem.at[r],
                device_id=d, device_id_type=LOGICAL,
            ).start()
        )

    def stats_wait(r):
        rest = st.at[r, pl.ds(0, n - 1)]
        pltpu.make_async_remote_copy(
            src_ref=rest, dst_ref=rest, send_sem=ss_sem.at[r], recv_sem=sr_sem.at[r],
            device_id=peer(1), device_id_type=LOGICAL,
        ).wait()
        return jnp.sum(st[r], axis=0)

    def pieces_send(w, phase):
        others(
            lambda d: pltpu.make_async_remote_copy(
                src_ref=pk.at[w, d] if phase == 0 else ags.at[w],
                dst_ref=(rsb if phase == 0 else agb).at[w, me],
                send_sem=ws_sem.at[w, phase], recv_sem=wr_sem.at[w, phase],
                device_id=d, device_id_type=LOGICAL,
            ).start()
        )

    def pieces_wait(w, phase):
        rest = (rsb if phase == 0 else agb).at[w, pl.ds(0, n - 1)]
        pltpu.make_async_remote_copy(
            src_ref=rest, dst_ref=rest,
            send_sem=ws_sem.at[w, phase], recv_sem=wr_sem.at[w, phase],
            device_id=peer(1), device_id_type=LOGICAL,
        ).wait()

    def kernel_products(vt, vo, vh):
        for j in range(3):
            g = jnp.concatenate([vo[j * R : (j + Y) * R, :], vh[j * R : (j + Y) * R, :]], axis=1)
            raw[j] = jnp.dot(vt[...], g, preferred_element_type=F32)

    def kernel_terms(w):
        block = lax.broadcasted_iota(jnp.int32, (C, L), 1) // C
        rows_v = cols_a + cols_b
        groups = [jnp.zeros((C, L), F32) for _ in range(7)]
        for j in range(3):
            dy = 2 - j
            for dx in range(3):
                for dz in range(3):
                    tap = dx * 9 + dy * 3 + dz
                    group, slot = tap // 4, tap % 4
                    for kb, (xv, zv) in enumerate(rows_v):
                        for cb, (xg, zg) in enumerate(rows_in):
                            if kb >= 4 and zv == 2 and zg != 1:
                                continue
                            if kb >= 4 and zv == -1 and zg != 0:
                                continue
                            if xv - xg + 1 != dx or zv - zg + 1 != dz:
                                continue
                            t, b = cb // 4, cb % 4
                            part = raw[j, kb * C : (kb + 1) * C, t * L : (t + 1) * L]
                            if slot != b:
                                part = pltpu.roll(part, (slot - b) % 4 * C, 1)
                            groups[group] = groups[group] + jnp.where(block == slot, part, 0.0)
        flat = jnp.concatenate(groups, axis=0)
        rows = n * PIECE
        if rows > flat.shape[0]:
            flat = jnp.concatenate([flat, jnp.zeros((rows - flat.shape[0], L), F32)], axis=0)
        pk[w] = flat.reshape(n, PIECE, L)
        rsb[w, me] = pk[w, me]

    def pieces_sum(w):
        pieces_wait(w, 0)
        whole = jnp.sum(rsb[w], axis=0).astype(BF16)
        ags[w] = whole
        agb[w, me] = whole
        pieces_send(w, 1)

    dk_refs = (dk1_ref, dk2_ref)

    def pieces_out(w):
        pieces_wait(w, 1)
        untap(agb[w].reshape(n * PIECE, L), dk_refs[w], total ** -0.5)

    def conv_rows(vo, vh, w_ref, c, slot=0):
        parts = []
        for j in range(3):
            rows = pl.ds(row_of(c * CH + j), CR)
            parts += [vo[rows, :], vh[rows, :]]
        ab = jnp.dot(
            jnp.concatenate(parts, axis=1), w_ref[...].reshape(6 * L, 2 * L),
            preferred_element_type=F32,
        )
        for k in range(CH):
            bs[slot + k, 8 : 8 + R, :] = ab[k * R : (k + 1) * R, L:]
        return [
            ab[k * R : (k + 1) * R, :L]
            + jnp.where(z0, bs[slot + k, 7 : 7 + R, :], bs[slot + k, 9 : 9 + R, :])
            for k in range(CH)
        ]

    def totals(vs):
        return fold(one(functools.reduce(jnp.add, [eight(v) for v in vs])))

    def center_near(s):
        mean = s / (4.0 * CR)
        high = mean.astype(BF16).astype(F32)
        low = (mean - high).astype(BF16).astype(F32)
        tile = jnp.concatenate(
            [jnp.broadcast_to(high, (8, L)), jnp.broadcast_to(low, (8, L))], axis=0
        )
        return high + low, tile

    cells = float(X * Y * Z)
    zero8 = jnp.zeros((8, L), F32)
    PAIR = 2

    def paired(e, step, carry, before=None, after=None):
        def group(i, carry, first):
            inner, s = carry
            if before is not None:
                before(i)
            found = []
            for k in range(PAIR):
                inner, vs = step(i * PAIR + k, k * CH, inner)
                found.append((vs, totals(vs)))
            if after is not None:
                after(i)
            center, tile = center_near(found[0][1] if first else s)
            for k, (vs, s) in enumerate(found):
                c = i * PAIR + k
                centers_of[e][pl.ds(c, 1), :] = center
                scs[pl.ds(c, 1), :] = s
                inner = keep_chunk(e, c, vs, center, tile, inner)
            if e != HID2 and i < early_groups(e):
                for k in range(PAIR):
                    send(e, i * PAIR + k, i < EARLY)
            return inner, s

        carry = group(0, (carry, None), True)
        for i in range(1, NCH // PAIR):
            carry = group(i, carry, False)
        return carry[0]

    EARLY = NCH // PAIR // 2

    def early_groups(e):
        return max(EARLY, NCH // PAIR - 1) if e == SLO1 else EARLY

    def send_late(e):
        for i in range(early_groups(e), NCH // PAIR):
            for k in range(PAIR):
                send(e, i * PAIR + k, i < EARLY)
        send_ends(e)

    centers_of = {HID1: mcs1, HID2: mcs, SLO1: mcs}

    def keep_chunk(e, c, vs, center, tile, inner):
        vs = [v - center for v in vs]
        pack(e, c, vs, tile)
        if e != SLO1:
            hc = hc1 if e == HID1 else hc2
            for k, v in enumerate(vs):
                hc[pl.ds(row_of(c * CH + k), R), :] = v
                inner = inner + eight(v * v)
        return inner

    def forward_loop(vo, vh, w_ref, e, before=None, after=None):
        def step(c, slot, squares):
            return squares, conv_rows(vo, vh, w_ref, c, slot)

        squares = fold(one(paired(e, step, zero8, before, after)))
        centers = centers_of[e][...]
        mean = one(scs[...]) / cells
        off = centers - mean
        rest = scs[...] - (4.0 * CR) * centers
        spread = squares + one(off * (2.0 * rest + (4.0 * CR) * off))
        return mean, spread

    def moments(r):
        sums = stats_wait(r)
        center = sums[0:1] / n

        off = st[r] - center
        between = jnp.sum(off * off, axis=0)[0:1]
        variance = (sums[1:2] + cells * between) / total
        return center, lax.rsqrt(variance + EPSILON)

    fetch[0].wait()

    def send_f(part):
        if part == 0:
            pl.semaphore_wait(barrier, n - 1)
        send_part(FEAT, part)

    enter(f_ref, vo_f, FEAT, send_f)
    send_ends(FEAT)
    fetch[1].wait()
    build(k1_ref, wf1, True)
    fetch[2].wait()
    build(k2_ref, wf2, True)
    build(k2_ref, wb2, False)
    build(k1_ref, wb1, False)
    fetch[3].wait()
    forward(FEAT, HALF)
    enter(c_ref, vo_c, COT)

    def put_f(dst):
        def use(row, value, center, keep):
            dst[pl.ds(row, R), :] = jnp.where(keep, value, 0.0).astype(BF16)

        return use

    arrive_ends(FEAT)
    each_end(FEAT, put_f(vh_f), put_f(vo_f))

    def take_f(c):
        found, _ = halo_rows(FEAT, c)
        for k, value in enumerate(found):
            put_f(vh_f)(row_of(c * CH + k + 1), value, None, keep_h)

    arrive(side_copies(FEAT, 0))
    take_f(0)

    def before_f(i):
        for c in range(i * PAIR + 1, min(i * PAIR + PAIR + 1, NCH)):
            arrive(side_copies(FEAT, c))
            take_f(c)

    mean, spread = forward_loop(vo_f, vh_f, wf1, HID1, before_f)
    stats_send(0, mean, spread)
    send_late(HID1)
    for copy in fetch[4:]:
        copy.wait()
    par[...] = jnp.zeros(par.shape, F32)
    for row, ref in enumerate((g1_ref, b1_ref, g2_ref, b2_ref)):
        par[row : row + 1, 0:C] = ref[...]
    params = fold(par[...])
    gain1, bias1, gain2, bias2 = [params[r : r + 1] for r in range(4)]
    flip(vo_f, vt_f)
    forward(HID1, HALF)
    center, inv1 = moments(0)
    send_all(COT)

    def put_a(n_dst, v_dst, inv, gain, bias, center):
        def use(row, value, mid, keep):
            normed = (value + (mid - center)) * inv
            n_dst[pl.ds(row, R), :] = normed
            a = activate(normed * gain + bias)
            v_dst[pl.ds(row, R), :] = (a if keep is None else jnp.where(keep, a, 0.0)).astype(BF16)

        return use

    own_a = put_a(n1o, vo_a, inv1, gain1, bias1, center)

    halo_a = put_a(n1h, vh_a, inv1, gain1, bias1, center)

    def active_own(c):
        mid = mcs1[c : c + 1, :]
        for k in range(CH):
            own_a(row_of(c * CH + k + 1), hc1[pl.ds(row_of(c * CH + k), R), :], mid, None)

    def active_halo(c):
        found, mid = halo_rows(HID1, c)
        for k, value in enumerate(found):
            halo_a(row_of(c * CH + k + 1), value, mid, keep_h)

    def after_a(i):
        for c in range(PAIR * (i + 1) + 1, min(PAIR * (i + 2) + 1, NCH)):
            active_own(c)
            active_halo(c)

    for c in range(min(PAIR + 1, NCH)):
        active_own(c)
    arrive_all(HID1)
    each_end(HID1, halo_a, own_a)
    for c in range(min(PAIR + 1, NCH)):
        active_halo(c)

    mean, spread = forward_loop(vo_a, vh_a, wf2, HID2, after=after_a)
    stats_send(1, mean, spread)
    flip(vo_a, vt_a)
    forward(COT, HALF)
    send_all(HID2)
    center, inv2 = moments(1)

    def own_output(c, carry):
        plain, along = carry
        mid = mcs[pl.ds(c, 1), :]
        for k in range(CH):
            y = c * CH + k
            normed = (hc2[pl.ds(row_of(y), R), :] + (mid - center)) * inv2
            shifted = normed * gain2 + bias2
            outb[pl.ds(row_of(y), R), :] = activate(shifted).astype(BF16)
            rows = pl.ds(row_of(y + 1), R)
            slope = vo_c[rows, :].astype(F32) * activate_slope(shifted)
            n2o[rows, :] = normed
            s2o[rows, :] = slope
            plain = plain + eight(slope)
            along = along + eight(slope * normed)
        return plain, along

    plain, along = lax.fori_loop(0, NCH, own_output, (zero8, zero8))
    stats_send(2, fold(one(plain)), fold(one(along)))

    forward(HID2, HALF)
    leave(outb, o_ref)
    arrive_all(COT)

    def put_c(dst):
        def use(row, value, mid, keep):
            dst[pl.ds(row, R), :] = value.astype(BF16)

        return use

    each_halo(COT, put_c(vh_c), put_c(vo_c))

    def put_s(n_dst, s_dst, c_src):
        def use(row, value, mid, keep):
            rows = pl.ds(row, R)
            normed = (value + (mid - center)) * inv2
            n_dst[rows, :] = normed
            s_dst[rows, :] = c_src[rows, :].astype(F32) * activate_slope(normed * gain2 + bias2)

        return use

    arrive_all(HID2)
    each_halo(HID2, put_s(n2h, s2h, vh_c), put_s(n2o, s2o, vo_c))
    sums2 = stats_wait(2)

    def gradient(slope, normed, sums, factor):
        return factor * (slope - sums[0:1] / total - normed * (sums[1:2] / total))

    factor2 = gain2 * inv2

    def grad_rows(row, keep_own, keep_halo):
        rows = pl.ds(row, R)
        g = gradient(s2o[rows, :], n2o[rows, :], sums2, factor2)
        vo_g[rows, :] = (g if keep_own is None else jnp.where(keep_own, g, 0.0)).astype(BF16)
        g = gradient(s2h[rows, :], n2h[rows, :], sums2, factor2)
        vh_g[rows, :] = jnp.where(keep_halo, g, 0.0).astype(BF16)

    def grad_two(c):
        for k in range(CH):
            grad_rows(row_of(c * CH + k + 1), None, keep_h)

    def after_g(i):
        for c in range(PAIR * (i + 1) + 1, min(PAIR * (i + 2) + 1, NCH)):
            grad_two(c)

    for c in range(min(PAIR + 1, NCH)):
        grad_two(c)
    for side in range(2):
        grad_rows(END[side] * R, keep_o[side], keep_ho[side])

    def back_step(c, slot, carry):
        plain, along = carry
        slopes = []
        for k, back in enumerate(conv_rows(vo_g, vh_g, wb2, c, slot)):
            rows = pl.ds(row_of(c * CH + k + 1), R)
            normed = n1o[rows, :]
            slope = back * activate_slope(normed * gain1 + bias1)
            s1o[rows, :] = slope
            plain = plain + eight(slope)
            along = along + eight(slope * normed)
            slopes.append(slope)
        return (plain, along), slopes

    plain, along = paired(SLO1, back_step, (zero8, zero8), after=after_g)
    stats_send(3, fold(one(plain)), fold(one(along)))
    send_late(SLO1)
    kernel_products(vt_a, vo_g, vh_g)
    forward(SLO1, HALF)
    kernel_terms(1)
    sums1 = stats_wait(3)
    factor1 = gain1 * inv1

    def put_g(dst, normed_ref):
        def use(row, value, mid, keep):
            rows = pl.ds(row, R)
            g = gradient(value + mid, normed_ref[rows, :], sums1, factor1)
            dst[rows, :] = jnp.where(keep, g, 0.0).astype(BF16)

        return use

    def grad_one(c, carry):
        for k in range(CH):
            rows = pl.ds(row_of(c * CH + k + 1), R)
            vo_g[rows, :] = gradient(s1o[rows, :], n1o[rows, :], sums1, factor1).astype(BF16)
        return carry

    lax.fori_loop(0, NCH, grad_one, 0)
    pieces_send(1, 0)
    arrive_all(SLO1)
    each_halo(SLO1, put_g(vh_g, n1h), put_g(vo_g, n1o))
    kernel_products(vt_f, vo_g, vh_g)
    kernel_terms(0)
    pieces_send(0, 0)

    def last_loop(i, carry):
        for j in range(PAIR):
            c = i * PAIR + j
            for k, back in enumerate(conv_rows(vo_g, vh_g, wb1, c, j * CH)):
                outb[pl.ds(row_of(c * CH + k), R), :] = back.astype(BF16)
        return carry

    for i in range(NCH // PAIR):
        last_loop(i, 0)
    pieces_sum(1)
    pieces_sum(0)
    leave(outb, fg_ref)
    for row, (sums, part) in enumerate(((sums1, 1), (sums1, 0), (sums2, 1), (sums2, 0))):
        ng_ref[row : row + 1, :] = sums[part : part + 1, 0:C] * total ** -0.5
    for e in range(NEXCH):
        sent_all(e)
        forwarded(e)
    pieces_out(1)
    pieces_out(0)


def finish(o_ref, fg_ref, dk1_ref, dk2_ref, ng_ref, *rest):
    outs, sem = rest[:-1], rest[-1]
    copies = [
        pltpu.make_async_copy(src, dst, sem.at[k])
        for k, (src, dst) in enumerate(zip((o_ref, fg_ref, dk1_ref, dk2_ref, ng_ref), outs))
    ]
    for copy in copies:
        copy.start()
    for copy in copies:
        copy.wait()


def local(features, kernel_one, gain_one, bias_one, kernel_two, gain_two, bias_two, cotangent):
    C, X, Y, Z = features.shape
    nx, ny = lax.axis_size("gx"), lax.axis_size("gy")
    n = nx * ny
    total = float(X * Y * Z * nx * ny)
    R = Z // 2
    NCH = Y // CH
    piece = -(-224 // (8 * n)) * 8
    taps = lambda k: jnp.transpose(k, (2, 3, 4, 0, 1)).reshape(27, C, C)
    row = lambda v: v.reshape(1, C)
    rows, all_rows = Y * R, (Y + 2) * R
    packed = CH * R // 2 + 16
    V = pltpu.VMEM
    DMA = pltpu.SemaphoreType.DMA
    scratch = [
        V((rows, L), F32), V((8, L), F32), V((R, 2 * Z), BF16), V((2 * L, 2 * Z), BF16),
        V((L, L), BF16), V((27, C, L), F32),
    ]
    scratch += [V((3, 2 * L, 2 * L), BF16)] * 4
    scratch += [V((all_rows, L), BF16)] * 8
    scratch += [V((2 * L, rows), BF16)] * 2
    scratch += [V((rows, L), F32)] * 2
    scratch += [V((all_rows, L), F32)] * 7
    scratch += [
        V((rows, L), BF16), V((2 * CH, R + 16, L), F32), V((NCH, L), F32), V((NCH, L), F32),
        V((NCH, L), F32), V((3, 2 * L, 2 * L), F32),
    ]
    scratch += [V((NEXCH, NCH, packed, L), BF16)] * 2 + [V((NEXCH, 3, R + 16, L), BF16)]
    scratch += [V((NEXCH, NCH, packed, L), BF16)] * 2 + [V((NEXCH, 2, R + 16, L), BF16)] * 3
    scratch += [DMA((NEXCH, 2 * NCH + 6))] * 2
    scratch += [V((4, 2, L), F32), V((4, n, 2, L), F32), DMA((4,)), DMA((4,))]
    scratch += [
        V((2, n, piece, L), F32), V((2, n, piece, L), F32), V((2, piece, L), BF16),
        V((2, n, piece, L), BF16), DMA((2, 2)), DMA((2, 2)),
        V((C, X, Y, Z), BF16), V((C, X, Y, Z), BF16), V((27, C, C), BF16), V((27, C, C), BF16),
        *[V((1, C), F32)] * 4, DMA((8,)), V((NEXCH, NCH // 2, packed, L), BF16),
        DMA((NEXCH, NCH // 2)), DMA((NEXCH, NCH // 2)),
    ]
    vmem = pl.BlockSpec(memory_space=pltpu.VMEM)
    anywhere = pl.BlockSpec(memory_space=pl.ANY)
    terms = jax.ShapeDtypeStruct((27, C, C), F32)
    volume = jax.ShapeDtypeStruct((C, X, Y, Z), BF16)
    mids = pl.pallas_call(
        functools.partial(kernel, nx, ny, total),
        name="blocks",
        out_shape=[
            volume, volume, terms, terms, jax.ShapeDtypeStruct((4, C), F32),
        ],
        in_specs=[pl.BlockSpec(memory_space=pltpu.HBM)] * 8,
        out_specs=[vmem] * 5,
        scratch_shapes=scratch,
        compiler_params=pltpu.CompilerParams(
            collective_id=0, has_side_effects=True, vmem_limit_bytes=48 << 20
        ),
    )(
        *[
            pltpu.with_memory_space_constraint(v, pltpu.HBM)
            for v in (
                features, cotangent, taps(kernel_one), taps(kernel_two),
                row(gain_one), row(bias_one), row(gain_two), row(bias_two),
            )
        ]
    )
    out, fg, dk1, dk2, norm = pl.pallas_call(
        finish,
        name="finish",
        out_shape=[volume, volume, terms, terms, jax.ShapeDtypeStruct((4, C), F32)],
        in_specs=[anywhere] * 5,
        out_specs=[anywhere] * 5,
        scratch_shapes=[DMA((5,))],
        compiler_params=pltpu.CompilerParams(vmem_limit_bytes=8 << 20),
    )(*mids)
    spatial = lambda d: jnp.transpose(d.reshape(3, 3, 3, C, C), (3, 4, 0, 1, 2))
    return out, fg, spatial(dk1), spatial(dk2), norm


def solution(mesh):
    in_specs = (P(None, "gx", "gy", None), P(), P(), P(), P(), P(), P(), P(None, "gx", "gy", None))
    out_specs = (P(None, "gx", "gy", None), P(None, "gx", "gy", None), P(), P(), P())
    return jax.shard_map(local, mesh=mesh, in_specs=in_specs, out_specs=out_specs, check_vma=False)
```
